256 devices in a mesh: rep: 1, dp: 256 (over x, y, z, core).
Axes of the slice: x: 4, y: 4, z: 8, core: 2. Of those that a mesh axis runs over, the one named last changes fastest.
Arguments:
- x: bfloat16 [256, 1024, 768], P(('rep', 'dp'))
- dy: bfloat16 [256, 1024, 768], P(('rep', 'dp'))
- w_gate: bfloat16 [2, 768, 2048], replicated
- w_up: bfloat16 [2, 768, 2048], replicated
- w_down: bfloat16 [2, 2048, 768], replicated
- m_w_gate: float32 [2, 768, 2048], replicated
- m_w_up: float32 [2, 768, 2048], replicated
- m_w_down: float32 [2, 2048, 768], replicated
- v_w_gate: float32 [2, 768, 2048], replicated
- v_w_up: float32 [2, 768, 2048], replicated
- v_w_down: float32 [2, 2048, 768], replicated
Outputs:
- output 1: bfloat16 [2, 768, 2048], P('rep')
- output 2: bfloat16 [2, 768, 2048], P('rep')
- output 3: bfloat16 [2, 2048, 768], P('rep')
- output 4: float32 [2, 768, 2048], P('rep')
- output 5: float32 [2, 768, 2048], P('rep')
- output 6: float32 [2, 2048, 768], P('rep')
- output 7: float32 [2, 768, 2048], P('rep')
- output 8: float32 [2, 768, 2048], P('rep')
- output 9: float32 [2, 2048, 768], P('rep')
All inputs are finite; a program needn't handle non-finite values.
Results may differ from the reference program's by a relative error of at most 0.022.
Values are sent between devices in bfloat16 or wider.
A program may use at most 768 MiB of HBM per device.

```python
import jax
import jax.numpy as jnp
from jax import lax

SEQUENCES = 256
TOKENS = 1024
D = 768
FF = 2048
LAYERS = 2
NAMES = ("w_gate", "w_up", "w_down")
SHAPES = {"w_gate": (LAYERS, D, FF), "w_up": (LAYERS, D, FF), "w_down": (LAYERS, FF, D)}


def bump(key, n, height):
    away = (jnp.arange(n, dtype=jnp.int32) - jax.random.randint(key, (), 0, n, jnp.int32)) % n
    return jnp.where(away < n // 8, height, 1.0)


def together(key, own, strength):
    shared = jax.random.normal(key, own.shape[1:], jnp.float32)
    return (own + strength * shared) * lax.rsqrt(1 + strength * strength)


def setup_inputs(seed: int = 0, part: int = 0) -> dict:
    kx, kdy, ka, kb, kz, kf, kh, kl, *keys = jax.random.split(jax.random.key(seed), 8 + 3 * len(NAMES))
    kx, kdy, ka, kb = (jax.random.fold_in(k, part) for k in (kx, kdy, ka, kb))
    kw, km, kv = (keys[i::3] for i in range(3))
    shape = (SEQUENCES, TOKENS, D)
    much_x, much_dy = jax.random.uniform(kz, (2,), jnp.float32, 0.0, 1.0)
    loud = 2.0 ** jax.random.uniform(jax.random.fold_in(kz, 1), (), jnp.float32, -1.0, 2.0)
    layers = 2.0 ** jax.random.uniform(kl, (LAYERS, 1, 1), jnp.float32, -1.0, 1.0)
    x = together(ka, jax.random.normal(kx, shape, jnp.float32), much_x) * bump(kf, D, 4.0)
    dy = together(kb, jax.random.normal(kdy, shape, jnp.float32), much_dy)
    drawn = {"x": x.astype(jnp.bfloat16), "dy": (loud * dy * (SEQUENCES * TOKENS) ** -0.5).astype(jnp.bfloat16)}
    for key, name in zip(kw, NAMES, strict=True):
        w = jax.random.normal(key, SHAPES[name], jnp.float32) * SHAPES[name][1] ** -0.5
        drawn[name] = (w * {"w_gate": 1.0, "w_up": bump(kh, FF, 4.0), "w_down": layers}[name]).astype(jnp.bfloat16)
    for key, name in zip(km, NAMES, strict=True):
        drawn[f"m_{name}"] = 0.1 * jax.random.normal(key, SHAPES[name], jnp.float32)
    for key, name in zip(kv, NAMES, strict=True):
        drawn[f"v_{name}"] = jax.random.uniform(key, SHAPES[name], jnp.float32, 0.005, 0.015)
    return drawn


def matmul(a, w):
    return jnp.dot(a, w, preferred_element_type=jnp.float32).astype(jnp.bfloat16)


def normed(h):
    wide = h.astype(jnp.float32)
    scale = lax.rsqrt(jnp.mean(wide**2, -1, keepdims=True) + 1e-6)
    return (wide * scale).astype(jnp.bfloat16)


def layer(h, w):
    a = normed(h)
    gate = jnp.dot(a, w["w_gate"], preferred_element_type=jnp.float32)
    up = jnp.dot(a, w["w_up"], preferred_element_type=jnp.float32)
    return h + matmul((jax.nn.silu(gate) * up).astype(jnp.bfloat16), w["w_down"])


def adamw(w, m, v, g):
    m = 0.9 * m + 0.1 * g
    v = 0.95 * v + 0.05 * g * g
    step = m * lax.rsqrt(v + 1e-8) + 0.1 * w
    return (w - 0.02 * step).astype(jnp.bfloat16), m, v


def clipped(gradients, sum_of_squares, count):
    factor = jnp.minimum(1.0, 0.5 * lax.rsqrt(sum_of_squares / count + 1e-30))
    return [g * factor for g in gradients]


def stack(weights, h):
    return lax.scan(lambda h, w: (layer(h, w), None), h, weights)[0]


def reference(x, dy, w_gate, w_up, w_down, m_w_gate, m_w_up, m_w_down, v_w_gate, v_w_up, v_w_down):
    weights = dict(zip(NAMES, (w_gate, w_up, w_down), strict=True))

    def take(so_far, sequence):
        h, by_y = sequence
        _, back = jax.vjp(lambda w: stack(w, h), weights)
        return jax.tree.map(lambda total, term: total + term.astype(jnp.float32), so_far, back(by_y)[0]), None

    none_yet = {name: jnp.zeros(w.shape, jnp.float32) for name, w in weights.items()}
    by_weights, _ = lax.scan(take, none_yet, (x, dy))
    gradients = [by_weights[name].astype(jnp.bfloat16).astype(jnp.float32) for name in NAMES]
    gradients = clipped(gradients, sum(jnp.sum(g * g) for g in gradients), sum(g.size for g in gradients))
    new = [
        adamw(w.astype(jnp.float32), m, v, g)
        for w, m, v, g in zip((w_gate, w_up, w_down), (m_w_gate, m_w_up, m_w_down), (v_w_gate, v_w_up, v_w_down), gradients, strict=True)
    ]
    return tuple(one[which] for which in range(3) for one in new)
```

```python
import functools

import jax
import jax.numpy as jnp
from jax import lax
from jax.experimental import pallas as pl
from jax.experimental.pallas import tpu as pltpu
from jax.sharding import PartitionSpec as P

NAMES = ("w_gate", "w_up", "w_down")
F32, BF16 = jnp.float32, jnp.bfloat16
MESH = pl.DeviceIdType.MESH
SLOTS = 8
LANES = 128


class Plan:
    def __init__(self, sizes, tiles, half):
        self.sizes, self.tiles, self.half = sizes, tiles, half
        nx, ny, nz = sizes
        self.axes = ((0, 1, 2), (1, 0, 2), (2, 0, 1))
        self.chunk = tuple(half // sizes[a[0]] for a in self.axes)
        self.piece = (half // (nx * ny), half // (nx * ny), 2 * half // (nz * nx))


STAGES = ("core", "r1", "r2", "r3", "r4", "p2", "p3", "b3", "b2", "a1", "a2", "a3", "a4", "out")


def rem(a, b):
    return lax.rem(a, jnp.int32(b))


def div(a, b):
    return lax.div(a, jnp.int32(b))


def comm_kernel(plan, *refs):
    sizes, tiles, half = plan.sizes, plan.tiles, plan.half
    grads, (g_out, squares), scratch = refs[:6], refs[6:8], refs[8:]
    g, mine, taken, s = scratch[:4]
    ring_in, ring_out = scratch[4:7], scratch[7:10]
    pair_in, pair_out, kept = scratch[10:13], scratch[13:16], scratch[16:19]
    own_in, own_out, own_kept = scratch[19:22], scratch[22:25], scratch[25:28]
    recv, send, local_sem, out_sem = scratch[28:]

    me = lax.axis_index("dp")
    core = rem(me, 2)
    at = [div(me, 2 * sizes[1] * sizes[2]), rem(div(me, 2 * sizes[2]), sizes[1]), rem(div(me, 2), sizes[2])]
    way = 1 - 2 * core

    def device(axis=None, place=None, other_core=False):
        c = [place if a == axis else at[a] for a in range(3)]
        return {"dp": ((c[0] * sizes[1] + c[1]) * sizes[2] + c[2]) * 2 + ((1 - core) if other_core else core)}

    def along(axis, step):
        return rem(at[axis] + step + 2 * sizes[axis], sizes[axis])

    def sem(array, color, stage, tile):
        return array.at[color, STAGES.index(stage), rem(tile, SLOTS)]

    def put(src, dst, color, stage, tile, where):
        pltpu.make_async_remote_copy(
            src_ref=src, dst_ref=dst, send_sem=sem(send, color, stage, tile), recv_sem=sem(recv, color, stage, tile),
            device_id=where, device_id_type=MESH,
        ).start()

    def wait(array, ref, color, stage, tile):
        pltpu.make_async_copy(ref, ref, sem(array, color, stage, tile)).wait()

    def part(color, tile, start, count):
        return g.at[tile, color, pl.ds(pl.multiple_of(start, 16), count), :]

    def some(tile, color, count):
        return g.at[tile, color, pl.ds(0, count), :]

    peers = [device(other_core=True)]
    for axis in range(3):
        peers += [device(axis, along(axis, step)) for step in range(1, sizes[axis])]
    barrier = pltpu.get_barrier_semaphore()
    for peer in peers:
        pl.semaphore_signal(barrier, inc=1, device_id=peer, device_id_type=MESH)
    pl.semaphore_wait(barrier, len(peers))

    def load(tile, start):
        for layer in range(2):

            @pl.when((tile >= (1 - layer) * (tiles // 2)) & (tile < (2 - layer) * (tiles // 2)))
            def _():
                for color in range(3):
                    for block in range(2):
                        column = pl.multiple_of(((rem(tile, tiles // 2)) * 2 + block) * LANES, LANES)
                        copy = pltpu.make_async_copy(
                            grads[3 * layer + color].at[:, pl.ds(column, LANES)],
                            mine.at[rem(tile, 4), color, pl.ds(block * half, half), :],
                            local_sem.at[rem(tile, 4), color, block],
                        )
                        copy.start() if start else copy.wait()

    def ring_sum(color, tile, step):
        axis = plan.axes[color][0]
        n, chunk = sizes[axis], plan.chunk[color]
        slot, far = rem(tile, SLOTS), n // 2 + 1 - step
        for direction in range(2 if step > 1 else 1):
            to = way if direction == 0 else -way
            rows = pl.ds(pl.multiple_of(along(axis, to * far) * chunk, 8), chunk)
            total = s[rem(tile, SLOTS), color, rows, :]
            if step > 1 + direction:
                total += ring_in[color][slot, step - 2, direction].astype(F32)
            ring_out[color][rem(slot, 2), step - 1, direction] = total.astype(BF16)
            put(ring_out[color].at[rem(slot, 2), step - 1, direction], ring_in[color].at[slot, step - 1, direction],
                color, f"r{step}", tile, device(axis, along(axis, to)))

    def ring_wait(array, color, tile, step):
        buffer = ring_in[color] if array is recv else ring_out[color]
        slot = rem(tile, SLOTS) if array is recv else rem(tile, 2)
        wait(array, buffer.at[slot, step - 1] if step > 1 else buffer.at[slot, 0, 0], color, f"r{step}", tile)

    def ring_end(color, tile):
        axis = plan.axes[color][0]
        n, chunk = sizes[axis], plan.chunk[color]
        rows = pl.ds(pl.multiple_of(at[axis] * chunk, 8), chunk)
        total = s[rem(tile, SLOTS), color, rows, :]
        for direction in range(2 if n > 2 else 1):
            total += ring_in[color][rem(tile, SLOTS), n // 2 - 1, direction].astype(F32)
        return total

    def exchange(color, tile, index):
        axis, piece = plan.axes[color][1], plan.piece[color]
        for step in range(1, sizes[axis]):
            owner = along(axis, step)
            rows = pl.ds(pl.multiple_of(owner * piece, 8), piece)
            pair_out[color][rem(index, 2), step - 1] = kept[color][rem(index, 2), rows, :].astype(BF16)
            put(pair_out[color].at[rem(index, 2), step - 1], pair_in[color].at[rem(index, SLOTS), step - 1], color, "p2", tile, device(axis, owner))

    def exchanged(color, tile, index):
        axis, last, piece = plan.axes[color][1], plan.axes[color][2], plan.piece[color]
        wait(recv, pair_in[color].at[rem(index, SLOTS)], color, "p2", tile)
        wait(send, pair_out[color].at[rem(index, 2)], color, "p2", tile)
        rows = pl.ds(pl.multiple_of(at[axis] * piece, 8), piece)
        total = kept[color][rem(index, 2), rows, :]
        for step in range(1, sizes[axis]):
            total += pair_in[color][rem(index, SLOTS), step - 1].astype(F32)
        owner = rem(index, sizes[last])

        @pl.when(at[last] != owner)
        def _():
            own_out[color][rem(index, 4)] = total.astype(BF16)
            put(own_out[color].at[rem(index, 4)], own_in[color].at[div(index, sizes[last]), rem(at[last] - owner + sizes[last], sizes[last]) - 1],
                color, "p3", tile, device(last, owner))

        @pl.when(at[last] == owner)
        def _():
            own_kept[color][rem(index, 4)] = total

    def place(color, tile):
        first, second = plan.axes[color][:2]
        chunk, piece = plan.chunk[color], plan.piece[color]
        base = core * half + at[first] * chunk
        return piece_place(color, tile, base, at[second], piece)

    def piece_place(color, tile, base, q, piece):
        if color < 2:
            return tile, base + q * piece
        per = plan.chunk[2] // piece
        return tile - 1 + div(q, per), base + rem(q, per) * piece

    def own_step(color, tile, index):
        last, piece = plan.axes[color][2], plan.piece[color]
        n = sizes[last]
        owner = rem(index, n)

        @pl.when(at[last] == owner)
        def _():
            wait(recv, own_in[color].at[div(index, n)], color, "p3", tile)
            total = own_kept[color][rem(index, 4)]
            for step in range(1, n):
                total += own_in[color][div(index, n), step - 1].astype(F32)
            where, row = place(color, tile)
            g[where, color, pl.ds(pl.multiple_of(row, 16), piece), :] = total.astype(BF16)
            for step in range(1, n):
                put(part_at(color, where, row, piece), part_at(color, where, row, piece), color, "b3", tile, device(last, along(last, step)))

        @pl.when(at[last] != owner)
        def _():
            wait(send, own_out[color].at[rem(index, 4)], color, "p3", tile)

    def part_at(color, tile, row, count):
        return g.at[tile, color, pl.ds(pl.multiple_of(row, 16), count), :]

    def spread(color, tile, index):
        second, last, piece = *plan.axes[color][1:], plan.piece[color]
        n = sizes[last]
        owner = rem(index, n)

        @pl.when(at[last] == owner)
        def _():
            wait(send, some(tile, color, (n - 1) * piece), color, "b3", tile)

        @pl.when(at[last] != owner)
        def _():
            wait(recv, some(tile, color, piece), color, "b3", tile)

        where, row = place(color, tile)
        for step in range(1, sizes[second]):
            put(part_at(color, where, row, piece), part_at(color, where, row, piece), color, "b2", tile, device(second, along(second, step)))

    def spread_wait(color, tile):
        count = (sizes[plan.axes[color][1]] - 1) * plan.piece[color]
        wait(recv, some(tile, color, count), color, "b2", tile)
        wait(send, some(tile, color, count), color, "b2", tile)

    def ring_gather(color, tile, step):
        axis, chunk = plan.axes[color][0], plan.chunk[color]
        n = sizes[axis]
        for direction in range(2 if step < n // 2 else 1):
            to = way if direction == 0 else -way
            row = core * half + along(axis, -to * (step - 1)) * chunk
            put(part_at(color, tile, row, chunk), part_at(color, tile, row, chunk), color, f"a{step}", tile, device(axis, along(axis, to)))

    def ring_gather_wait(color, tile, step):
        axis, chunk = plan.axes[color][0], plan.chunk[color]
        count = (2 if step < sizes[axis] // 2 else 1) * chunk
        wait(recv, some(tile, color, count), color, f"a{step}", tile)
        wait(send, some(tile, color, count), color, f"a{step}", tile)

    def core_gather(color, tile):
        put(part_at(color, tile, core * half, half), part_at(color, tile, core * half, half), color, "out", tile, device(other_core=True))

    def finish(color, tile):
        wait(recv, some(tile, color, half), color, "out", tile)
        wait(send, some(tile, color, half), color, "out", tile)
        pltpu.make_async_copy(g.at[tile, color], g_out.at[tile, color], out_sem.at[color, rem(tile, 2)]).start()
        values = g[tile, color].astype(F32).reshape(2 * half // 8, 8, LANES)
        squares[tile, color] = jnp.sum(values * values, axis=0)

    def finished(color, tile):
        pltpu.make_async_copy(g.at[tile, color], g_out.at[tile, color], out_sem.at[color, rem(tile, 2)]).wait()

    rings = [sizes[a[0]] // 2 for a in plan.axes]
    jobs = []

    def core_send(tile):
        load(tile, False)
        put(mine.at[rem(tile, 4), :, pl.ds(pl.multiple_of((1 - core) * half, 16), half), :], taken.at[rem(tile, SLOTS)], 0, "core", tile, device(other_core=True))

    def core_take(tile):
        wait(recv, taken.at[rem(tile, SLOTS)], 0, "core", tile)
        wait(send, taken.at[rem(tile, SLOTS)], 0, "core", tile)
        for color in range(3):
            own = mine[rem(tile, 4), color, pl.ds(pl.multiple_of(core * half, 16), half), :]
            s[rem(tile, SLOTS), color] = own.astype(F32) + taken[rem(tile, SLOTS), color].astype(F32)
            ring_sum(color, tile, 1)

    def ring_next(color, step):
        def job(tile):
            ring_wait(recv, color, tile, step - 1)
            ring_wait(send, color, tile, step - 1)
            ring_sum(color, tile, step)
        return job

    def ring_last(color):
        def job(tile):
            ring_wait(recv, color, tile, rings[color])
            ring_wait(send, color, tile, rings[color])
            if color < 2:
                kept[color][rem(tile, 2)] = ring_end(color, tile)
                exchange(color, tile, tile)
            else:
                chunk = plan.chunk[color]
                kept[color][rem(div(tile, 2), 2), pl.ds(pl.multiple_of((rem(tile, 2)) * chunk, 8), chunk), :] = ring_end(color, tile)
        return job

    index_of = lambda color, tile: tile if color < 2 else div(tile, 2)
    jobs.append((0, 0, core_send))
    jobs.append((1, 0, core_take))
    late = {}
    for color in range(3):
        odd = color == 2
        for step in range(2, rings[color] + 1):
            jobs.append((step, 0, ring_next(color, step)))
        end = rings[color] + 1
        jobs.append((end, 0, ring_last(color)))
        if odd:
            jobs.append((end, 1, lambda tile: exchange(2, tile, div(tile, 2))))
        jobs.append((end + 1, odd, lambda tile, c=color: exchanged(c, tile, index_of(c, tile))))
        jobs.append((end + 3, odd, lambda tile, c=color: own_step(c, tile, index_of(c, tile))))
        jobs.append((end + 5, odd, lambda tile, c=color: spread(c, tile, index_of(c, tile))))
        jobs.append((end + 6, odd, lambda tile, c=color: spread_wait(c, tile)))
        begin = end + 6 + (1 if odd else 0)
        for step in range(1, rings[color] + 1):
            def gather(tile, c=color, step=step):
                if step > 1:
                    ring_gather_wait(c, tile, step - 1)
                ring_gather(c, tile, step)
            jobs.append((begin + step - 1, 0, gather))

        def gathered(tile, c=color):
            ring_gather_wait(c, tile, rings[c])
            core_gather(c, tile)
        jobs.append((begin + rings[color], 0, gathered))
        jobs.append((begin + rings[color] + 1, 0, lambda tile, c=color: finish(c, tile)))
        jobs.append((begin + rings[color] + 2, 0, lambda tile, c=color: finished(c, tile)))
    jobs.sort(key=lambda job: job[0])
    ticks = tiles + jobs[-1][0]

    for tile in range(2):
        load(tile, True)

    def tick(now, carry):
        @pl.when(now + 2 < tiles)
        def _():
            load(now + 2, True)

        for delay, odd, job in jobs:
            tile = now - delay
            there = (tile >= 0) & (tile < tiles)
            if odd:
                there &= rem(tile, 2) == 1
            pl.when(there)(functools.partial(job, tile))
        return carry

    lax.fori_loop(0, ticks, tick, 0)


def all_reduce(plan, grads):
    sizes, tiles, half, chunk, piece = plan.sizes, plan.tiles, plan.half, plan.chunk, plan.piece
    n1 = [sizes[a[0]] for a in plan.axes]
    n2 = [sizes[a[1]] for a in plan.axes]
    n3 = [sizes[a[2]] for a in plan.axes]
    owned = [-(-(tiles if c < 2 else tiles // 2) // n3[c]) for c in range(3)]
    vmem = pltpu.VMEM
    scratch = [
        vmem((tiles, 3, 2 * half, LANES), BF16),
        vmem((4, 3, 2 * half, LANES), BF16),
        vmem((SLOTS, 3, half, LANES), BF16),
        vmem((SLOTS, 3, half, LANES), F32),
    ]
    scratch += [vmem((SLOTS, n1[c] // 2, 2, chunk[c], LANES), BF16) for c in range(3)]
    scratch += [vmem((2, n1[c] // 2, 2, chunk[c], LANES), BF16) for c in range(3)]
    scratch += [vmem((SLOTS, n2[c] - 1, piece[c], LANES), BF16) for c in range(3)]
    scratch += [vmem((2, n2[c] - 1, piece[c], LANES), BF16) for c in range(3)]
    scratch += [vmem((2, n2[c] * piece[c], LANES), F32) for c in range(3)]
    scratch += [vmem((owned[c], n3[c] - 1, piece[c], LANES), BF16) for c in range(3)]
    scratch += [vmem((4, piece[c], LANES), BF16) for c in range(3)]
    scratch += [vmem((4, piece[c], LANES), F32) for c in range(3)]
    dma = pltpu.SemaphoreType.DMA
    scratch += [dma((3, len(STAGES), SLOTS)), dma((3, len(STAGES), SLOTS)), dma((4, 3, 2)), dma((3, 2))]
    return pl.pallas_call(
        functools.partial(comm_kernel, plan),
        name="sum_gradients",
        out_shape=(
            jax.ShapeDtypeStruct((tiles, 3, 2 * half, LANES), BF16),
            jax.ShapeDtypeStruct((tiles, 3, 8, LANES), F32),
        ),
        in_specs=[pl.BlockSpec(memory_space=pl.ANY)] * 6,
        out_specs=(pl.BlockSpec(memory_space=pl.ANY), pl.BlockSpec(memory_space=pltpu.VMEM)),
        scratch_shapes=scratch,
        compiler_params=pltpu.CompilerParams(collective_id=0, has_side_effects=True, vmem_limit_bytes=67_000_000),
    )(*grads)


def adamw_kernel(count, g_ref, squares_ref, *refs):
    ws, ms, vs, new_ws, new_ms, new_vs = (refs[i : i + 3] for i in range(0, 18, 3))
    factor = jnp.minimum(1.0, 0.5 * lax.rsqrt(jnp.sum(squares_ref[...]) / count + 1e-30))
    for color in range(3):
        half = g_ref.shape[2] // 2
        for block in range(2):
            g = g_ref[0, color, pl.ds(block * half, half), :].astype(F32)
            if color == 2:
                g = g.T
                rows, columns = pl.ds(block * LANES, LANES), pl.ds(0, half)
            else:
                rows, columns = pl.ds(0, half), pl.ds(block * LANES, LANES)
            g = g * factor
            m = 0.9 * ms[color][0, rows, columns] + 0.1 * g
            v = 0.95 * vs[color][0, rows, columns] + 0.05 * g * g
            w = ws[color][0, rows, columns].astype(F32)
            new_ws[color][0, rows, columns] = (w - 0.02 * (m * lax.rsqrt(v + 1e-8) + 0.1 * w)).astype(BF16)
            new_ms[color][0, rows, columns] = m
            new_vs[color][0, rows, columns] = v


def adamw(g, squares, weights, m, v):
    tiles = g.shape[0]
    half = g.shape[2] // 2
    per = tiles // 2
    up = pl.BlockSpec((1, half, 2 * LANES), lambda i: (1 - i // per, 0, i % per))
    down = pl.BlockSpec((1, 2 * LANES, half), lambda i: (1 - i // per, i % per, 0))
    three = [up, up, down]
    out = [jax.ShapeDtypeStruct(a.shape, a.dtype) for a in (*weights, *m, *v)]
    return pl.pallas_call(
        functools.partial(adamw_kernel, float(sum(w.size for w in weights))),
        name="adamw",
        grid=(tiles,),
        out_shape=out,
        in_specs=[pl.BlockSpec((1, 3, 2 * half, LANES), lambda i: (i, 0, 0, 0)), pl.BlockSpec(squares.shape, lambda i: (0,) * 4)] + three * 3,
        out_specs=three * 3,
        compiler_params=pltpu.CompilerParams(vmem_limit_bytes=62_000_000),
    )(g, squares, *weights, *m, *v)


def matmul(a, w):
    return jnp.dot(a, w, preferred_element_type=jnp.float32).astype(jnp.bfloat16)


def normed(h):
    wide = h.astype(jnp.float32)
    scale = lax.rsqrt(jnp.mean(wide**2, -1, keepdims=True) + 1e-6)
    return (wide * scale).astype(jnp.bfloat16)


def layer(h, w):
    a = normed(h)
    gate = jnp.dot(a, w["w_gate"], preferred_element_type=jnp.float32)
    up = jnp.dot(a, w["w_up"], preferred_element_type=jnp.float32)
    return h + matmul((jax.nn.silu(gate) * up).astype(jnp.bfloat16), w["w_down"].T)


def solution(mesh):
    plan = Plan((4, 4, 8), 16, 768)

    def step(x, dy, *arrays):
        weights, m, v = (arrays[i : i + 3] for i in (0, 3, 6))
        layers = weights[0].shape[0]
        of = [{"w_gate": weights[0][n], "w_up": weights[1][n], "w_down": weights[2][n].T} for n in range(layers)]
        h, kept = x[0], []
        for number in range(layers):
            kept.append(h)
            h = layer(h, of[number])
        by_h, grads = dy[0], [None] * layers
        for number in reversed(range(layers)):
            _, back = jax.vjp(lambda w, h: layer(h, w), of[number], kept[number])
            by_w, by_h = back(by_h)
            grads[number] = [by_w[name] for name in NAMES]
        g, squares = all_reduce(plan, grads[0] + grads[1])
        return tuple(adamw(g, squares, weights, m, v))

    return jax.shard_map(
        step,
        mesh=mesh,
        in_specs=(P(("rep", "dp"), None, None),) * 2 + (P(None, None, None),) * 9,
        out_specs=(P("rep", None, None),) * 9,
        check_vma=False,
    )
```

```python
import functools

import jax
import jax.numpy as jnp
from jax import lax
from jax.experimental import pallas as pl
from jax.experimental.pallas import tpu as pltpu
from jax.sharding import PartitionSpec as P

F32, BF16 = jnp.float32, jnp.bfloat16
MESH = pl.DeviceIdType.MESH
SLOTS = 8
W = 256
LANES = 128


class Plan:
    def __init__(self, sizes, tiles, half):
        self.sizes, self.tiles, self.half = sizes, tiles, half
        nx, ny, nz = sizes
        self.axes = ((0, 1, 2), (1, 0, 2), (2, 0, 1))
        self.chunk = tuple(half // sizes[a[0]] for a in self.axes)
        self.piece = (half // (nx * ny), half // (nx * ny), 2 * half // (nz * nx))


STAGES = ("core", "r1", "r2", "r3", "r4", "p2", "p3", "b3", "b2", "a1", "a2", "a3", "a4", "out")


def rem(a, b):
    return lax.rem(a, jnp.int32(b))


def div(a, b):
    return lax.div(a, jnp.int32(b))


def dot(a, b, dims=((1,), (0,))):
    return lax.dot_general(a, b, (dims, ((), ())), preferred_element_type=F32)


LAST = ((1,), (1,))


def normed(h):
    wide = h.astype(F32)
    return (wide * lax.rsqrt(jnp.mean(wide * wide, -1, keepdims=True) + 1e-6)).astype(BF16)


def train_kernel(plan, *refs):
    sizes, tiles, half = plan.sizes, plan.tiles, plan.half
    x_hbm, dy_hbm, gate_hbm, up_hbm, down_hbm = refs[:5]
    g_out, squares = refs[5:7]
    scratch = list(refs[7:])

    def take(count):
        out, scratch[:] = scratch[:count], scratch[count:]
        return out

    g, mine, taken, s = take(4)
    ring_in, ring_out, pair_in, pair_out, kept, own_in, own_out, own_kept = (take(3) for _ in range(8))
    sq, = take(1)
    recv, send, out_sem, sq_recv, sq_send_sem = take(5)
    h, d, a0, a1, at_, dt, acc, p, dg, du, down_all, wg, wu, wd, in_sem, w_sem = take(16)
    tokens, width = h.shape
    per = tiles // 2
    rows = min(256, tokens)

    me = lax.axis_index("dp")
    core = rem(me, 2)
    at = [div(me, 2 * sizes[1] * sizes[2]), rem(div(me, 2 * sizes[2]), sizes[1]), rem(div(me, 2), sizes[2])]
    way = 1 - 2 * core

    def device(axis=None, place=None, other_core=False):
        c = [place if a == axis else at[a] for a in range(3)]
        return {"dp": ((c[0] * sizes[1] + c[1]) * sizes[2] + c[2]) * 2 + ((1 - core) if other_core else core)}

    def along(axis, step):
        return rem(at[axis] + step + 2 * sizes[axis], sizes[axis])


    def fetch(layer, t, slot, start, down=True):
        cols = pl.ds(pl.multiple_of(t * W, W), W)
        copies = [(gate_hbm.at[layer, :, cols], wg.at[slot]), (up_hbm.at[layer, :, cols], wu.at[slot])]
        if down:
            copies.append((down_hbm.at[layer, cols, :], wd.at[slot]))
        for i, (src, dst) in enumerate(copies):
            copy = pltpu.make_async_copy(src, dst, w_sem.at[slot, i])
            copy.start() if start else copy.wait()

    def fetch_tile(q, start):
        for layer in range(2):
            first = (1 - layer) * per

            @pl.when((q >= first) & (q < first + per))
            def _():
                fetch(layer, q - first, rem(q, 4), start)

    def tile_forward(slot, a, d):
        for r in range(0, tokens, rows):
            block = pl.ds(r, rows)
            gate = dot(a[block, :], wg[slot])
            up = dot(a[block, :], wu[slot])
            by_p = dot(d[block, :], wd[slot], LAST).astype(BF16).astype(F32)
            sig = jax.nn.sigmoid(gate)
            act = gate * sig
            p[block, 0:W] = (act * up).astype(BF16)
            du[block, :] = (by_p * act).astype(BF16)
            dg[block, :] = (by_p * up * (sig * (1 + gate * (1 - sig)))).astype(BF16)

    def tile_gradients(tile, dt):
        for color, (left, right) in enumerate(((at_, dg), (at_, du), (dt, p))):
            out = dot(left[...], right[:, 0:W])
            low, high = out[:, :LANES], out[:, LANES:]
            s[rem(tile, S_SLOTS), color] = jnp.where(core == 0, low, high)
            mine[rem(tile, 2), color] = jnp.where(core == 0, high, low).astype(BF16)

    def tile_by_input(slot):
        for r in range(0, tokens, rows):
            block = pl.ds(r, rows)
            acc[block, :] += dot(dg[block, :], wg[slot], LAST) + dot(du[block, :], wu[slot], LAST)

    def through_norm():
        for r in range(0, tokens, rows):
            block = pl.ds(r, rows)
            wide = h[block, :].astype(F32)
            scale = lax.rsqrt(jnp.mean(wide * wide, -1, keepdims=True) + 1e-6)
            by_a = acc[block, :].astype(BF16).astype(F32)
            by_h = by_a * scale - wide * (scale * scale * scale * (jnp.sum(by_a * wide, -1, keepdims=True) * (1.0 / width)))
            d[block, :] = (d[block, :].astype(F32) + by_h.astype(BF16).astype(F32)).astype(BF16)

    def forward():
        load_x = pltpu.make_async_copy(x_hbm.at[0], h, in_sem.at[0])
        load_dy = pltpu.make_async_copy(dy_hbm.at[0], d, in_sem.at[1])
        load_down = pltpu.make_async_copy(down_hbm.at[0], down_all, in_sem.at[2])
        load_x.start()
        for t in range(2):
            fetch(0, t, t, True, False)
        load_down.start()
        load_dy.start()
        load_x.wait()
        for r in range(0, tokens, rows):
            a0[r : r + rows, :] = normed(h[r : r + rows, :])

        def pair(i, carry):
            base = 2 * rem(i, 2)
            for k in range(2):
                fetch(0, 2 * i + k, base + k, False, False)

            @pl.when(i + 1 < per // 2)
            def _():
                for k in range(2):
                    fetch(0, 2 * i + 2 + k, 2 - base + k, True, False)

            @pl.when(i + 1 == per // 2)
            def _():
                fetch(1, 0, 2 - base, True)

            for k in range(2):
                for r in range(0, tokens, rows):
                    gate = dot(a0[r : r + rows, :], wg[base + k])
                    up = dot(a0[r : r + rows, :], wu[base + k])
                    p[r : r + rows, pl.ds(pl.multiple_of((2 * i + k) * W, W), W)] = (gate * jax.nn.sigmoid(gate) * up).astype(BF16)
            return carry

        lax.fori_loop(0, per // 2, pair, 0)
        load_down.wait()
        for r in range(0, tokens, rows):
            made = dot(p[r : r + rows, :], down_all[...]).astype(BF16).astype(F32)
            out = (h[r : r + rows, :].astype(F32) + made).astype(BF16)
            h[r : r + rows, :] = out
            a1[r : r + rows, :] = normed(out)
        at_[...] = a1[...].T
        acc[...] = jnp.zeros_like(acc)
        load_dy.wait()
        dt[...] = d[...].T
        fetch_tile(jnp.int32(0), False)
        fetch_tile(jnp.int32(1), True)
        tile_forward(0, a1, d)

    def compute(tile):
        slot, after = rem(tile, 4), rem(tile + 1, 4)

        @pl.when(tile + 1 < tiles)
        def _():
            fetch_tile(tile + 1, False)

        @pl.when(tile + 2 < tiles)
        def _():
            fetch_tile(tile + 2, True)

        @pl.when(tile < per - 1)
        def _():
            tile_gradients(tile, dt)
            tile_by_input(slot)
            tile_forward(after, a1, d)

        @pl.when(tile == per - 1)
        def _():
            tile_by_input(slot)
            tile_gradients(tile, dt)
            through_norm()
            at_[...] = a0[...].T
            dt[...] = d[...].T
            tile_forward(after, a0, d)

        @pl.when((tile >= per) & (tile < tiles - 1))
        def _():
            tile_gradients(tile, dt)
            tile_forward(after, a0, d)

        @pl.when(tile == tiles - 1)
        def _():
            tile_gradients(tile, dt)


    def sem(array, color, stage, tile):
        return array.at[color, STAGES.index(stage), rem(tile, SLOTS)]

    def put(src, dst, color, stage, tile, where):
        pltpu.make_async_remote_copy(
            src_ref=src, dst_ref=dst, send_sem=sem(send, color, stage, tile), recv_sem=sem(recv, color, stage, tile),
            device_id=where, device_id_type=MESH,
        ).start()

    def wait(array, ref, color, stage, tile):
        pltpu.make_async_copy(ref, ref, sem(array, color, stage, tile)).wait()

    def some(tile, color, count):
        return g.at[tile, color, pl.ds(0, count), :]

    def part_at(color, tile, row, count):
        return g.at[tile, color, pl.ds(pl.multiple_of(row, 16), count), :]

    def ring_sum(color, tile, step):
        axis = plan.axes[color][0]
        n, chunk = sizes[axis], plan.chunk[color]
        slot, out, far = rem(tile, R_SLOTS), rem(tile, 2), n // 2 + 1 - step
        for direction in range(2 if step > 1 else 1):
            to = way if direction == 0 else -way
            lines = pl.ds(pl.multiple_of(along(axis, to * far) * chunk, 8), chunk)
            total = s[rem(tile, S_SLOTS), color, lines, :]
            if step > 1 + direction:
                total += ring_in[color][slot, step - 2, direction].astype(F32)
            ring_out[color][out, step - 1, direction] = total.astype(BF16)
            put(ring_out[color].at[out, step - 1, direction], ring_in[color].at[slot, step - 1, direction],
                color, f"r{step}", tile, device(axis, along(axis, to)))

    def ring_wait(color, tile, step):
        for array, buffer, slot in ((recv, ring_in[color], rem(tile, R_SLOTS)), (send, ring_out[color], rem(tile, 2))):
            wait(array, buffer.at[slot, step - 1] if step > 1 else buffer.at[slot, 0, 0], color, f"r{step}", tile)

    def ring_end(color, tile):
        axis = plan.axes[color][0]
        n, chunk = sizes[axis], plan.chunk[color]
        lines = pl.ds(pl.multiple_of(at[axis] * chunk, 8), chunk)
        total = s[rem(tile, S_SLOTS), color, lines, :]
        for direction in range(2 if n > 2 else 1):
            total += ring_in[color][rem(tile, R_SLOTS), n // 2 - 1, direction].astype(F32)
        return total

    def exchange(color, tile, index):
        axis, piece = plan.axes[color][1], plan.piece[color]
        for step in range(1, sizes[axis]):
            owner = along(axis, step)
            lines = pl.ds(pl.multiple_of(owner * piece, 8), piece)
            pair_out[color][rem(index, 2), step - 1] = kept[color][rem(index, 2), lines, :].astype(BF16)
            put(pair_out[color].at[rem(index, 2), step - 1], pair_in[color].at[rem(index, R_SLOTS), step - 1], color, "p2", tile, device(axis, owner))

    def exchanged(color, tile, index):
        axis, last, piece = plan.axes[color][1], plan.axes[color][2], plan.piece[color]
        wait(recv, pair_in[color].at[rem(index, R_SLOTS)], color, "p2", tile)
        wait(send, pair_out[color].at[rem(index, 2)], color, "p2", tile)
        lines = pl.ds(pl.multiple_of(at[axis] * piece, 8), piece)
        total = kept[color][rem(index, 2), lines, :]
        for step in range(1, sizes[axis]):
            total += pair_in[color][rem(index, R_SLOTS), step - 1].astype(F32)
        owner = rem(index, sizes[last])

        @pl.when(at[last] != owner)
        def _():
            own_out[color][rem(index, 4)] = total.astype(BF16)
            put(own_out[color].at[rem(index, 4)], own_in[color].at[div(index, sizes[last]), rem(at[last] - owner + sizes[last], sizes[last]) - 1],
                color, "p3", tile, device(last, owner))

        @pl.when(at[last] == owner)
        def _():
            own_kept[color][rem(index, 4)] = total

    def place(color, tile):
        first, second = plan.axes[color][:2]
        chunk, piece, q = plan.chunk[color], plan.piece[color], at[second]
        base = core * half + at[first] * chunk
        if color < 2:
            return tile, base + q * piece
        count = chunk // piece
        return tile - 1 + div(q, count), base + rem(q, count) * piece

    def own_step(color, tile, index):
        last, piece = plan.axes[color][2], plan.piece[color]
        n = sizes[last]
        owner = rem(index, n)

        @pl.when(at[last] == owner)
        def _():
            wait(recv, own_in[color].at[div(index, n)], color, "p3", tile)
            total = own_kept[color][rem(index, 4)]
            for step in range(1, n):
                total += own_in[color][div(index, n), step - 1].astype(F32)
            final = total.astype(BF16)
            where, row = place(color, tile)
            g[where, color, pl.ds(pl.multiple_of(row, 16), piece), :] = final
            for step in range(1, n):
                put(part_at(color, where, row, piece), part_at(color, where, row, piece), color, "b3", tile, device(last, along(last, step)))
            wide = final.astype(F32)
            mine_sq = sq.at[0, at[SQ_AXES[0]]]
            mine_sq[...] += jnp.sum((wide * wide).reshape(piece // 8, 8, LANES), axis=0)

        @pl.when(at[last] != owner)
        def _():
            wait(send, own_out[color].at[rem(index, 4)], color, "p3", tile)

    def spread(color, tile, index):
        second, last, piece = *plan.axes[color][1:], plan.piece[color]
        n = sizes[last]
        owner = rem(index, n)

        @pl.when(at[last] == owner)
        def _():
            wait(send, some(tile, color, (n - 1) * piece), color, "b3", tile)

        @pl.when(at[last] != owner)
        def _():
            wait(recv, some(tile, color, piece), color, "b3", tile)

        where, row = place(color, tile)
        for step in range(1, sizes[second]):
            put(part_at(color, where, row, piece), part_at(color, where, row, piece), color, "b2", tile, device(second, along(second, step)))

    def spread_wait(color, tile):
        count = (sizes[plan.axes[color][1]] - 1) * plan.piece[color]
        wait(recv, some(tile, color, count), color, "b2", tile)
        wait(send, some(tile, color, count), color, "b2", tile)

    def ring_gather(color, tile, step):
        axis, chunk = plan.axes[color][0], plan.chunk[color]
        n = sizes[axis]
        for direction in range(2 if step < n // 2 else 1):
            to = way if direction == 0 else -way
            row = core * half + along(axis, -to * (step - 1)) * chunk
            put(part_at(color, tile, row, chunk), part_at(color, tile, row, chunk), color, f"a{step}", tile, device(axis, along(axis, to)))

    def ring_gather_wait(color, tile, step):
        axis, chunk = plan.axes[color][0], plan.chunk[color]
        count = (2 if step < sizes[axis] // 2 else 1) * chunk
        wait(recv, some(tile, color, count), color, f"a{step}", tile)
        wait(send, some(tile, color, count), color, f"a{step}", tile)

    def core_gather(color, tile):
        put(part_at(color, tile, core * half, half), part_at(color, tile, core * half, half), color, "out", tile, device(other_core=True))

    def finish(color, tile):
        wait(recv, some(tile, color, half), color, "out", tile)
        wait(send, some(tile, color, half), color, "out", tile)
        pltpu.make_async_copy(g.at[tile, color], g_out.at[tile, color], out_sem.at[color, rem(tile, 2)]).start()

    def finished(color, tile):
        pltpu.make_async_copy(g.at[tile, color], g_out.at[tile, color], out_sem.at[color, rem(tile, 2)]).wait()

    def core_send(tile):
        put(mine.at[rem(tile, 2)], taken.at[rem(tile, 4)], 0, "core", tile, device(other_core=True))

    def core_take(tile):
        wait(recv, taken.at[rem(tile, 4)], 0, "core", tile)
        wait(send, taken.at[rem(tile, 4)], 0, "core", tile)
        for color in range(3):
            s[rem(tile, S_SLOTS), color] += taken[rem(tile, 4), color].astype(F32)
            ring_sum(color, tile, 1)

    def sq_peers(level):
        if level == 3:
            return [(core, device(other_core=True))]
        axis = SQ_AXES[level]
        return [(at[axis], device(axis, along(axis, step))) for step in range(1, sizes[axis])]

    def sq_send(level):
        for index, peer in sq_peers(level):
            pltpu.make_async_remote_copy(
                src_ref=sq.at[level, index], dst_ref=sq.at[level, index], send_sem=sq_send_sem.at[level], recv_sem=sq_recv.at[level],
                device_id=peer, device_id_type=MESH,
            ).start()

    def sq_take(level):
        count = len(sq_peers(level))
        for array in (sq_recv, sq_send_sem):
            ref = sq.at[level, pl.ds(0, count)]
            pltpu.make_async_copy(ref, ref, array.at[level]).wait()
        total = sq[level, 0]
        for i in range(1, count + 1):
            total += sq[level, i]
        if level == 3:
            squares[...] = total
        else:
            sq[level + 1, (at[SQ_AXES[level + 1]] if level < 2 else core)] = total
            sq_send(level + 1)

    rings = [sizes[a[0]] // 2 for a in plan.axes]

    def index_of(color, tile):
        return tile if color < 2 else div(tile, 2)

    def ring_next(color, step):
        def job(tile):
            ring_wait(color, tile, step - 1)
            ring_sum(color, tile, step)
        return job

    def ring_last(color):
        def job(tile):
            ring_wait(color, tile, rings[color])
            if color < 2:
                kept[color][rem(tile, 2)] = ring_end(color, tile)
                exchange(color, tile, tile)
            else:
                chunk = plan.chunk[color]
                kept[color][rem(div(tile, 2), 2), pl.ds(pl.multiple_of(rem(tile, 2) * chunk, 8), chunk), :] = ring_end(color, tile)
        return job

    ALL, ODD, FINAL = range(3)
    jobs = []
    for color in range(3):
        which = ODD if color == 2 else ALL
        for step in range(2, rings[color] + 1):
            jobs.append((step + 1, ALL, ring_next(color, step)))
        end = rings[color] + 2
        jobs.append((end, ALL, ring_last(color)))
        if color == 2:
            jobs.append((end, ODD, lambda tile: exchange(2, tile, div(tile, 2))))
        jobs.append((end + 1, which, lambda tile, c=color: exchanged(c, tile, index_of(c, tile))))
        jobs.append((end + 3, which, lambda tile, c=color: own_step(c, tile, index_of(c, tile))))
        jobs.append((end + 5, which, lambda tile, c=color: spread(c, tile, index_of(c, tile))))
        jobs.append((end + 6, which, lambda tile, c=color: spread_wait(c, tile)))
        begin = end + 6 + (1 if color == 2 else 0)
        for step in range(1, rings[color] + 1):
            def gather(tile, c=color, step=step):
                if step > 1:
                    ring_gather_wait(c, tile, step - 1)
                ring_gather(c, tile, step)
            jobs.append((begin + step - 1, ALL, gather))

        def gathered(tile, c=color):
            ring_gather_wait(c, tile, rings[c])
            core_gather(c, tile)
        jobs.append((begin + rings[color], ALL, gathered))
        jobs.append((begin + rings[color] + 1, ALL, lambda tile, c=color: finish(c, tile)))
        jobs.append((begin + rings[color] + 2, ALL, lambda tile, c=color: finished(c, tile)))
    summed = max(rings) + 2 + 3
    jobs.append((summed, FINAL, lambda tile: sq_send(0)))
    for level in range(4):
        jobs.append((summed + 1 + level, FINAL, lambda tile, level=level: sq_take(level)))
    jobs.sort(key=lambda job: job[0])
    ticks = tiles + jobs[-1][0]

    peers = [device(other_core=True)]
    for axis in range(3):
        peers += [device(axis, along(axis, step)) for step in range(1, sizes[axis])]
    barrier = pltpu.get_barrier_semaphore()
    for peer in peers:
        pl.semaphore_signal(barrier, inc=1, device_id=peer, device_id_type=MESH)
    sq[...] = jnp.zeros_like(sq)
    forward()
    pl.semaphore_wait(barrier, len(peers))

    def tick(now, carry):
        for delay, which, job in jobs:
            tile = now - delay
            there = (tile >= 0) & (tile < tiles) if which != FINAL else tile == tiles - 1
            if which == ODD:
                there &= rem(tile, 2) == 1
            pl.when(there)(functools.partial(job, tile))

        @pl.when(now < tiles)
        def _():
            compute(now)
            core_send(now)

        @pl.when((now >= 1) & (now <= tiles))
        def _():
            core_take(now - 1)
        return carry

    lax.fori_loop(0, ticks, tick, 0)


S_SLOTS, R_SLOTS = 6, 4
SQ_AXES = (2, 1, 0)


def gradients(plan, x, dy, weights):
    sizes, tiles, half, chunk, piece = plan.sizes, plan.tiles, plan.half, plan.chunk, plan.piece
    n1, n2, n3 = ([sizes[a[i]] for a in plan.axes] for i in range(3))
    owned = [-(-(tiles if c < 2 else tiles // 2) // n3[c]) for c in range(3)]
    tokens, width = x.shape[1:]
    hidden = tiles // 2 * W
    vmem, dma = pltpu.VMEM, pltpu.SemaphoreType.DMA
    scratch = [
        vmem((tiles, 3, 2 * half, LANES), BF16),
        vmem((2, 3, half, LANES), BF16),
        vmem((4, 3, half, LANES), BF16),
        vmem((S_SLOTS, 3, half, LANES), F32),
    ]
    scratch += [vmem((R_SLOTS, n1[c] // 2, 2, chunk[c], LANES), BF16) for c in range(3)]
    scratch += [vmem((2, n1[c] // 2, 2, chunk[c], LANES), BF16) for c in range(3)]
    scratch += [vmem((R_SLOTS, n2[c] - 1, piece[c], LANES), BF16) for c in range(3)]
    scratch += [vmem((2, n2[c] - 1, piece[c], LANES), BF16) for c in range(3)]
    scratch += [vmem((2, n2[c] * piece[c], LANES), F32) for c in range(3)]
    scratch += [vmem((owned[c], n3[c] - 1, piece[c], LANES), BF16) for c in range(3)]
    scratch += [vmem((4, piece[c], LANES), BF16) for c in range(3)]
    scratch += [vmem((4, piece[c], LANES), F32) for c in range(3)]
    scratch += [vmem((4, 8, 8, LANES), F32)]
    scratch += [dma((3, len(STAGES), SLOTS)), dma((3, len(STAGES), SLOTS)), dma((3, 2)), dma((4,)), dma((4,))]
    state, turned = vmem((tokens, width), BF16), vmem((width, tokens), BF16)
    scratch += [state, state, state, state, turned, turned, vmem((tokens, width), F32)]
    scratch += [vmem((tokens, hidden), BF16), vmem((tokens, W), BF16), vmem((tokens, W), BF16), vmem((hidden, width), BF16)]
    scratch += [vmem((4, width, W), BF16), vmem((4, width, W), BF16), vmem((4, W, width), BF16), dma((3,)), dma((4, 3))]
    flops = 34 * tokens * width * hidden
    return pl.pallas_call(
        functools.partial(train_kernel, plan),
        name="gradients",
        out_shape=(jax.ShapeDtypeStruct((tiles, 3, 2 * half, LANES), BF16), jax.ShapeDtypeStruct((8, LANES), F32)),
        in_specs=[pl.BlockSpec(memory_space=pl.ANY)] * 5,
        out_specs=(pl.BlockSpec(memory_space=pl.ANY), pl.BlockSpec(memory_space=pltpu.VMEM)),
        scratch_shapes=scratch,
        cost_estimate=pl.CostEstimate(flops=flops, bytes_accessed=12 * width * hidden * 2, transcendentals=0),
        compiler_params=pltpu.CompilerParams(collective_id=0, has_side_effects=True, vmem_limit_bytes=67_000_000),
    )(x, dy, *weights)


def adamw_kernel(count, squares_ref, *refs):
    gs, ws, ms, vs, new_ws, new_ms, new_vs = (refs[i : i + 3] for i in range(0, 21, 3))
    factor = jnp.minimum(1.0, 0.5 * lax.rsqrt(jnp.sum(squares_ref[...]) / count + 1e-30))

    def update(color, g, rows, columns):
        g = g.astype(F32) * factor
        m = 0.9 * ms[color][0, rows, columns] + 0.1 * g
        v = 0.95 * vs[color][0, rows, columns] + 0.05 * g * g
        w = ws[color][0, rows, columns].astype(F32)
        new_ws[color][0, rows, columns] = (w - 0.02 * (m * lax.rsqrt(v + 1e-8) + 0.1 * w)).astype(BF16)
        new_ms[color][0, rows, columns] = m
        new_vs[color][0, rows, columns] = v

    for color in range(2):
        for t in range(gs[color].shape[0]):
            for block in range(2):
                update(color, gs[color][t, 0, block], slice(None), pl.ds((2 * t + block) * LANES, LANES))
    for block in range(2):
        update(2, gs[2][0, 0, block].astype(F32).T, pl.ds(block * LANES, LANES), slice(None))


def adamw(g, squares, weights, m, v):
    tiles, _, half = g.shape[0], 0, g.shape[2] // 2
    per = tiles // 2
    g = g.reshape(tiles, 3, 2, half, LANES)
    lines = half // per
    up = pl.BlockSpec((1, lines, W * per), lambda i: (1 - i // per, i % per, 0))
    down = pl.BlockSpec((1, W, half), lambda i: (1 - i // per, i % per, 0))
    three = [up, up, down]
    by = [pl.BlockSpec((per, 1, 2, lines, LANES), lambda i, c=c: (i // per, c, 0, i % per, 0)) for c in range(2)]
    by.append(pl.BlockSpec((1, 1, 2, half, LANES), lambda i: (i, 2, 0, 0, 0)))
    out = [jax.ShapeDtypeStruct(a.shape, a.dtype) for a in (*weights, *m, *v)]
    return pl.pallas_call(
        functools.partial(adamw_kernel, float(sum(w.size for w in weights))),
        name="adamw",
        grid=(tiles,),
        out_shape=out,
        in_specs=[pl.BlockSpec(squares.shape, lambda i: (0, 0))] + by + three * 3,
        out_specs=three * 3,
        compiler_params=pltpu.CompilerParams(vmem_limit_bytes=62_000_000),
    )(squares, g, g, g, *weights, *m, *v)


def solution(mesh):
    plan = Plan((4, 4, 8), 16, 768)

    def step(x, dy, *arrays):
        weights, m, v = (arrays[i : i + 3] for i in (0, 3, 6))
        g, squares = gradients(plan, x, dy, weights)
        return tuple(adamw(g, squares, weights, m, v))

    return jax.shard_map(
        step,
        mesh=mesh,
        in_specs=(P(("rep", "dp"), None, None),) * 2 + (P(None, None, None),) * 9,
        out_specs=(P("rep", None, None),) * 9,
        check_vma=False,
    )
```

```python
import functools

import jax
import jax.numpy as jnp
from jax import lax
from jax.experimental import pallas as pl
from jax.experimental.pallas import tpu as pltpu
from jax.sharding import PartitionSpec as P

F32, BF16 = jnp.float32, jnp.bfloat16
MESH = pl.DeviceIdType.MESH
SLOTS = 4
W = 256
LANES = 128


def ring_steps(n):
    half = n // 2
    sums = [[(1, half + 1 - k, 0 if k > 1 else None)] + ([(-1, k - half - 1, 1 if k > 2 else None)] if k > 1 else []) for k in range(1, half + 1)]
    copies = [[(1, 1 - k)] + ([(-1, k - 1)] if k < half else []) for k in range(1, half + 1)]
    return sums, copies


class Plan:
    def __init__(self, sizes, tiles, half):
        self.sizes, self.tiles, self.half = sizes, tiles, half
        groups = [((0, (0, 1, 2)), (1, (1, 0, 2))), ((2, (2, 0, 1)),)]
        self.members, self.span, self.sums, self.copies = [], [], [], []
        self.length, self.chunk, self.piece, self.owners, self.keys = [], [], [], [], [(0, "core")]
        for members in groups:
            n1, n2, n3 = (sizes[a] for a in members[0][1])
            assert all(tuple(sizes[a] for a in axes) == (n1, n2, n3) for _, axes in members)
            sums, copies = ring_steps(n1)
            self.members.append(members)
            self.span.append((0, tiles))
            self.sums.append(sums)
            self.copies.append(copies)
            self.length.append((n1, n2, n3))
            self.chunk.append(half // n1)
            self.piece.append(half // (n1 * n2))
            self.owners.append(half // (n1 * n2) // 8)
            self.keys += [(len(self.span) - 1, f"{c}{k + 1}") for c in "ra" for k in range(len(sums))]
            self.keys += [(len(self.span) - 1, name) for name in ("p2", "p3", "b3", "b2", "out")]


def rem(a, b):
    return lax.rem(a, jnp.int32(b))


def div(a, b):
    return lax.div(a, jnp.int32(b))


def dot(a, b, dims=((1,), (0,))):
    return lax.dot_general(a, b, (dims, ((), ())), preferred_element_type=F32)


LAST = ((1,), (1,))


def normed(h):
    wide = h.astype(F32)
    return (wide * lax.rsqrt(jnp.mean(wide * wide, -1, keepdims=True) + 1e-6)).astype(BF16)


def train_kernel(plan, *refs):
    sizes, tiles, half = plan.sizes, plan.tiles, plan.half
    x_hbm, dy_hbm, gate_hbm, up_hbm, down_hbm = refs[:5]
    g, squares = refs[5:7]
    scratch = list(refs[7:])

    def take(count):
        out, scratch[:] = scratch[:count], scratch[count:]
        return out

    mine, taken, s = take(3)
    ring_in, ring_out, pair_in, pair_out, kept, own_in, own_out, own_kept = (take(len(plan.span)) for _ in range(8))
    sq, = take(1)
    recv, send, sq_recv, sq_send_sem = take(4)
    h, d, a0, a1, at_, dt, acc, p, dg, du, down_all, wg, wu, wd, in_sem, w_sem = take(16)
    tokens, width = h.shape
    per = tiles // 2
    rows = min(256, tokens)

    me = lax.axis_index("dp")
    core = rem(me, 2)
    at = [div(me, 2 * sizes[1] * sizes[2]), rem(div(me, 2 * sizes[2]), sizes[1]), rem(div(me, 2), sizes[2])]
    way = 1 - 2 * core

    def device(axis=None, place=None, other_core=False):
        c = [place if a == axis else at[a] for a in range(3)]
        return {"dp": ((c[0] * sizes[1] + c[1]) * sizes[2] + c[2]) * 2 + ((1 - core) if other_core else core)}

    def along(axis, step):
        return rem(at[axis] + step + 2 * sizes[axis], sizes[axis])


    def fetch(layer, t, slot, start, down=True):
        cols = pl.ds(pl.multiple_of(t * W, W), W)
        copies = [(gate_hbm.at[layer, :, cols], wg.at[slot]), (up_hbm.at[layer, :, cols], wu.at[slot])]
        if down:
            copies.append((down_hbm.at[layer, cols, :], wd.at[slot]))
        for i, (src, dst) in enumerate(copies):
            copy = pltpu.make_async_copy(src, dst, w_sem.at[slot, i])
            copy.start() if start else copy.wait()

    def fetch_tile(q, start):
        for layer in range(2):
            first = (1 - layer) * per

            @pl.when((q >= first) & (q < first + per))
            def _():
                fetch(layer, q - first, rem(q, 4), start)

    def tile_forward(slot, a, d):
        for r in range(0, tokens, rows):
            block = pl.ds(r, rows)
            gate = dot(a[block, :], wg[slot])
            up = dot(a[block, :], wu[slot])
            by_p = dot(d[block, :], wd[slot], LAST).astype(BF16).astype(F32)
            sig = jax.nn.sigmoid(gate)
            act = gate * sig
            p[block, 0:W] = (act * up).astype(BF16)
            du[block, :] = (by_p * act).astype(BF16)
            dg[block, :] = (by_p * up * (sig * (1 + gate * (1 - sig)))).astype(BF16)

    def tile_gradients(tile, dt):
        for color, (left, right) in enumerate(((at_, dg), (at_, du), (dt, p))):
            out = dot(left[...], right[:, 0:W])
            low, high = out[:, :LANES], out[:, LANES:]
            s[rem(tile, S_SLOTS), color] = jnp.where(core == 0, low, high)
            mine[rem(tile, 2), color] = jnp.where(core == 0, high, low).astype(BF16)

    def tile_by_input(slot):
        for r in range(0, tokens, rows):
            block = pl.ds(r, rows)
            acc[block, :] += dot(dg[block, :], wg[slot], LAST) + dot(du[block, :], wu[slot], LAST)

    def through_norm():
        for r in range(0, tokens, rows):
            block = pl.ds(r, rows)
            wide = h[block, :].astype(F32)
            scale = lax.rsqrt(jnp.mean(wide * wide, -1, keepdims=True) + 1e-6)
            by_a = acc[block, :].astype(BF16).astype(F32)
            by_h = by_a * scale - wide * (scale * scale * scale * (jnp.sum(by_a * wide, -1, keepdims=True) * (1.0 / width)))
            d[block, :] = (d[block, :].astype(F32) + by_h.astype(BF16).astype(F32)).astype(BF16)

    def forward():
        load_x = pltpu.make_async_copy(x_hbm.at[0], h, in_sem.at[0])
        load_dy = pltpu.make_async_copy(dy_hbm.at[0], d, in_sem.at[1])
        load_down = pltpu.make_async_copy(down_hbm.at[0], down_all, in_sem.at[2])
        load_x.start()
        for t in range(2):
            fetch(0, t, t, True, False)
        load_down.start()
        load_dy.start()
        load_x.wait()
        for r in range(0, tokens, rows):
            a0[r : r + rows, :] = normed(h[r : r + rows, :])

        def pair(i, carry):
            base = 2 * rem(i, 2)
            for k in range(2):
                fetch(0, 2 * i + k, base + k, False, False)

            @pl.when(i + 1 < per // 2)
            def _():
                for k in range(2):
                    fetch(0, 2 * i + 2 + k, 2 - base + k, True, False)

            @pl.when(i + 1 == per // 2)
            def _():
                fetch(1, 0, 2 - base, True)

            for k in range(2):
                for r in range(0, tokens, rows):
                    gate = dot(a0[r : r + rows, :], wg[base + k])
                    up = dot(a0[r : r + rows, :], wu[base + k])
                    p[r : r + rows, pl.ds(pl.multiple_of((2 * i + k) * W, W), W)] = (gate * jax.nn.sigmoid(gate) * up).astype(BF16)
            return carry

        lax.fori_loop(0, per // 2, pair, 0)
        load_down.wait()
        for r in range(0, tokens, rows):
            made = dot(p[r : r + rows, :], down_all[...]).astype(BF16).astype(F32)
            out = (h[r : r + rows, :].astype(F32) + made).astype(BF16)
            h[r : r + rows, :] = out
            a1[r : r + rows, :] = normed(out)
        at_[...] = a1[...].T
        acc[...] = jnp.zeros_like(acc)
        load_dy.wait()
        dt[...] = d[...].T
        fetch_tile(jnp.int32(0), False)
        fetch_tile(jnp.int32(1), True)
        tile_forward(0, a1, d)

    def gradients_of(tile):
        tile_gradients(tile, dt)

    def rest(tile):
        slot, after = rem(tile, 4), rem(tile + 1, 4)

        @pl.when(tile + 1 < tiles)
        def _():
            fetch_tile(tile + 1, False)

        @pl.when(tile + 2 < tiles)
        def _():
            fetch_tile(tile + 2, True)

        @pl.when(tile < per - 1)
        def _():
            tile_by_input(slot)
            tile_forward(after, a1, d)

        @pl.when(tile == per - 1)
        def _():
            tile_by_input(slot)
            through_norm()
            at_[...] = a0[...].T
            dt[...] = d[...].T
            tile_forward(after, a0, d)

        @pl.when((tile >= per) & (tile < tiles - 1))
        def _():
            tile_forward(after, a0, d)


    def sem(array, group, stage, tile):
        return array.at[plan.keys.index((group, stage)), rem(tile, SLOTS)]

    def put(src, dst, group, stage, tile, where):
        pltpu.make_async_remote_copy(
            src_ref=src, dst_ref=dst, send_sem=sem(send, group, stage, tile), recv_sem=sem(recv, group, stage, tile),
            device_id=where, device_id_type=MESH,
        ).start()

    def wait(array, ref, group, stage, tile):
        pltpu.make_async_copy(ref, ref, sem(array, group, stage, tile)).wait()

    def some(group, tile, count):
        return g.at[tile, plan.members[group][0][0], pl.ds(0, count * len(plan.members[group])), :]

    def spot(weight, tile, row, count):
        return g.at[tile, weight, pl.ds(pl.multiple_of(row, 8), count), :]

    def eight(row, count):
        return pl.ds(pl.multiple_of(row, 8), count)

    def first_sends(group, tile, step):
        slot, out, chunk = rem(tile, R_SLOTS), rem(tile, 2), plan.chunk[group]
        for m, (weight, axes) in enumerate(plan.members[group]):
            for i, (to, whose, before) in enumerate(plan.sums[group][step - 1]):
                total = s[rem(tile, S_SLOTS), weight, eight(along(axes[0], way * whose) * chunk, chunk), :]
                if before is not None:
                    total += ring_in[group][slot, step - 2, before, m].astype(F32)
                ring_out[group][out, step - 1, i, m] = total.astype(BF16)
                put(ring_out[group].at[out, step - 1, i, m], ring_in[group].at[slot, step - 1, i, m], group, f"r{step}", tile,
                    device(axes[0], along(axes[0], way * to)))

    def first_wait(group, tile, step):
        count = len(plan.sums[group][step - 1])
        wait(recv, ring_in[group].at[rem(tile, R_SLOTS), step - 1, pl.ds(0, count)], group, f"r{step}", tile)
        wait(send, ring_out[group].at[rem(tile, 2), step - 1, pl.ds(0, count)], group, f"r{step}", tile)

    def first_next(group, tile, step):
        first_wait(group, tile, step - 1)
        first_sends(group, tile, step)

    def first_last(group, tile):
        steps, chunk, piece, slot = len(plan.sums[group]), plan.chunk[group], plan.piece[group], rem(tile, 2)
        first_wait(group, tile, steps)
        for m, (weight, axes) in enumerate(plan.members[group]):
            total = s[rem(tile, S_SLOTS), weight, eight(at[axes[0]] * chunk, chunk), :]
            for i in range(len(plan.sums[group][-1])):
                total += ring_in[group][rem(tile, R_SLOTS), steps - 1, i, m].astype(F32)
            kept[group][slot, m] = total
            for k in range(1, sizes[axes[1]]):
                owner = along(axes[1], k)
                pair_out[group][slot, k - 1, m] = kept[group][slot, m, eight(owner * piece, piece), :].astype(BF16)
                put(pair_out[group].at[slot, k - 1, m], pair_in[group].at[rem(tile, R_SLOTS), k - 1, m], group, "p2", tile, device(axes[1], owner))

    def exchanged(group, tile):
        piece, slot, n = plan.piece[group], rem(tile, 4), plan.length[group][2]
        wait(recv, pair_in[group].at[rem(tile, R_SLOTS)], group, "p2", tile)
        wait(send, pair_out[group].at[rem(tile, 2)], group, "p2", tile)
        for m, (weight, axes) in enumerate(plan.members[group]):
            total = kept[group][rem(tile, 2), m, eight(at[axes[1]] * piece, piece), :]
            for k in range(1, sizes[axes[1]]):
                total += pair_in[group][rem(tile, R_SLOTS), k - 1, m].astype(F32)
            own_kept[group][slot, m] = total
            own_out[group][slot, m] = total.astype(BF16)
        last = plan.members[group][0][1][2]
        for owner in range(plan.owners[group]):

            @pl.when(at[last] != owner)
            def _():
                put(own_out[group].at[slot, :, pl.ds(8 * owner, 8)], own_in[group].at[slot, rem(at[last] + (n - 1 - owner), n)],
                    group, "p3", tile, device(last, jnp.int32(owner)))

    def place(group, axes):
        return core * half + at[axes[0]] * plan.chunk[group] + at[axes[1]] * plan.piece[group]

    def own_step(group, tile):
        n, slot, last = plan.length[group][2], rem(tile, 4), plan.members[group][0][1][2]

        @pl.when(at[last] < plan.owners[group])
        def _():
            wait(recv, own_in[group].at[slot], group, "p3", tile)
            for m, (weight, axes) in enumerate(plan.members[group]):
                total = own_kept[group][slot, m, eight(8 * at[last], 8), :]
                for k in range(1, n):
                    total += own_in[group][slot, k - 1, m].astype(F32)
                final = total.astype(BF16)
                row = place(group, axes) + 8 * at[last]
                g[tile, weight, eight(row, 8), :] = final
                for k in range(1, n):
                    put(spot(weight, tile, row, 8), spot(weight, tile, row, 8), group, "b3", tile, device(last, along(last, k)))
                wide = final.astype(F32)
                mine_sq = sq.at[0, at[SQ_AXES[0]]]
                mine_sq[...] += wide * wide

        line_wait(send, group, tile, "p3")

    def line_wait(array, group, tile, stage):
        owners, last = plan.owners[group], plan.members[group][0][1][2]
        if owners > 1:

            @pl.when(at[last] < owners)
            def _():
                wait(array, some(group, tile, 8 * (owners - 1)), group, stage, tile)

        if owners < sizes[last]:

            @pl.when(at[last] >= owners)
            def _():
                wait(array, some(group, tile, 8 * owners), group, stage, tile)

    def spread(group, tile):
        last, piece = plan.members[group][0][1][2], plan.piece[group]

        @pl.when(at[last] < plan.owners[group])
        def _():
            wait(send, some(group, tile, (plan.length[group][2] - 1) * 8), group, "b3", tile)

        line_wait(recv, group, tile, "b3")
        for weight, axes in plan.members[group]:
            row = place(group, axes)
            for k in range(1, sizes[axes[1]]):
                put(spot(weight, tile, row, piece), spot(weight, tile, row, piece), group, "b2", tile, device(axes[1], along(axes[1], k)))

    def gather(group, tile, step):
        chunk = plan.chunk[group]
        if step == 1:
            for array in (recv, send):
                wait(array, some(group, tile, (plan.length[group][1] - 1) * plan.piece[group]), group, "b2", tile)
        else:
            gather_wait(group, tile, step - 1)
        for weight, axes in plan.members[group]:
            for to, whose in plan.copies[group][step - 1]:
                row = core * half + along(axes[0], way * whose) * chunk
                put(spot(weight, tile, row, chunk), spot(weight, tile, row, chunk), group, f"a{step}", tile, device(axes[0], along(axes[0], way * to)))

    def gather_wait(group, tile, step):
        for array in (recv, send):
            wait(array, some(group, tile, len(plan.copies[group][step - 1]) * plan.chunk[group]), group, f"a{step}", tile)

    def both(group):
        weights = [weight for weight, _ in plan.members[group]]
        return pl.ds(weights[0], len(weights))

    def gathered(group, tile):
        gather_wait(group, tile, len(plan.copies[group]))
        mine_half = g.at[tile, both(group), eight(core * half, half), :]
        put(mine_half, mine_half, group, "out", tile, device(other_core=True))

    def finish(group, tile):
        for array in (recv, send):
            wait(array, some(group, tile, half), group, "out", tile)

    def core_send(tile):
        put(mine.at[rem(tile, 2)], taken.at[rem(tile, 2)], 0, "core", tile, device(other_core=True))

    def core_take(tile):
        wait(recv, taken.at[rem(tile, 2)], 0, "core", tile)
        wait(send, taken.at[rem(tile, 2)], 0, "core", tile)
        for weight in range(3):
            s[rem(tile, S_SLOTS), weight] += taken[rem(tile, 2), weight].astype(F32)

    def sq_peers(level):
        if level == 3:
            return [(core, device(other_core=True))]
        axis = SQ_AXES[level]
        return [(at[axis], device(axis, along(axis, step))) for step in range(1, sizes[axis])]

    def sq_send(level):
        for index, peer in sq_peers(level):
            pltpu.make_async_remote_copy(
                src_ref=sq.at[level, index], dst_ref=sq.at[level, index], send_sem=sq_send_sem.at[level], recv_sem=sq_recv.at[level],
                device_id=peer, device_id_type=MESH,
            ).start()

    def sq_take(level):
        count = len(sq_peers(level))
        for array in (sq_recv, sq_send_sem):
            ref = sq.at[level, pl.ds(0, count)]
            pltpu.make_async_copy(ref, ref, array.at[level]).wait()
        total = sq[level, 0]
        for i in range(1, count + 1):
            total += sq[level, i]
        if level == 3:
            squares[...] = total
        else:
            sq[level + 1, (at[SQ_AXES[level + 1]] if level < 2 else core)] = total
            sq_send(level + 1)

    jobs = [(1, 0, 0, tiles, core_take)]
    for group in range(len(plan.span)):
        def add(delay, part, job, *rest, group=group):
            jobs.append((delay, part, *plan.span[group], lambda tile: job(group, tile, *rest)))

        steps = len(plan.sums[group])
        add(1, 0, first_sends, 1)
        for step in range(2, steps + 1):
            add(step, 0, first_next, step)
        add(steps + 1, 0, first_last)
        add(steps + 2, 0, exchanged)
        own = steps + (4 if plan.length[group][2] > 4 else 3)
        add(own, 0, own_step)
        add(own + 1, 1, spread)
        for step in range(1, steps + 1):
            add(own + 1 + step, 1, gather, step)
        add(own + 2 + steps, 1, gathered)
        add(own + 3 + steps, 1, finish)
    summed = max(job[0] + job[3] - tiles for job in jobs if job[1] == 0)
    jobs.append((summed, 0, tiles - 1, tiles, lambda tile: sq_send(0)))
    for level in range(4):
        jobs.append((summed + 1 + level, 1, tiles - 1, tiles, lambda tile, level=level: sq_take(level)))
    jobs.sort(key=lambda job: job[0])
    ticks = max(job[0] + job[3] for job in jobs)

    peers = [device(other_core=True)]
    for axis in range(3):
        peers += [device(axis, along(axis, step)) for step in range(1, sizes[axis])]
    barrier = pltpu.get_barrier_semaphore()
    for peer in peers:
        pl.semaphore_signal(barrier, inc=1, device_id=peer, device_id_type=MESH)
    sq[...] = jnp.zeros_like(sq)
    forward()
    pl.semaphore_wait(barrier, len(peers))

    def run(now, some_jobs):
        for delay, _, first, end, job in some_jobs:
            tile = now - delay
            pl.when((tile >= first) & (tile < end))(functools.partial(job, tile))

    def tick(now, carry):
        for part in range(2):
            here = [job for job in jobs if job[1] == part]
            pl.when(now >= min(job[0] + job[2] for job in here))(functools.partial(run, now, here))

            @pl.when(now < tiles)
            def _():
                if part:
                    rest(now)
                else:
                    gradients_of(now)
                    core_send(now)
        return carry

    lax.fori_loop(0, ticks, tick, 0)


S_SLOTS, R_SLOTS = 5, 4
SQ_AXES = (2, 1, 0)


def gradients(plan, x, dy, weights):
    tiles, half, chunk, piece = plan.tiles, plan.half, plan.chunk, plan.piece
    tokens, width = x.shape[1:]
    hidden = tiles // 2 * W
    vmem, dma = pltpu.VMEM, pltpu.SemaphoreType.DMA
    scratch = [
        vmem((2, 3, half, LANES), BF16),
        vmem((2, 3, half, LANES), BF16),
        vmem((S_SLOTS, 3, half, LANES), F32),
    ]
    groups = range(len(plan.span))
    count = [len(members) for members in plan.members]
    most = [max(len(step) for step in sums) for sums in plan.sums]
    scratch += [vmem((R_SLOTS, len(plan.sums[c]), most[c], count[c], chunk[c], LANES), BF16) for c in groups]
    scratch += [vmem((2, len(plan.sums[c]), most[c], count[c], chunk[c], LANES), BF16) for c in groups]
    scratch += [vmem((R_SLOTS, plan.length[c][1] - 1, count[c], piece[c], LANES), BF16) for c in groups]
    scratch += [vmem((2, plan.length[c][1] - 1, count[c], piece[c], LANES), BF16) for c in groups]
    scratch += [vmem((2, count[c], chunk[c], LANES), F32) for c in groups]
    scratch += [vmem((4, plan.length[c][2] - 1, count[c], 8, LANES), BF16) for c in groups]
    scratch += [vmem((4, count[c], piece[c], LANES), BF16) for c in groups]
    scratch += [vmem((4, count[c], piece[c], LANES), F32) for c in groups]
    scratch += [vmem((4, 8, 8, LANES), F32)]
    scratch += [dma((len(plan.keys), SLOTS)), dma((len(plan.keys), SLOTS)), dma((4,)), dma((4,))]
    state, turned = vmem((tokens, width), BF16), vmem((width, tokens), BF16)
    scratch += [state, state, state, state, turned, turned, vmem((tokens, width), F32)]
    scratch += [vmem((tokens, hidden), BF16), vmem((tokens, W), BF16), vmem((tokens, W), BF16), vmem((hidden, width), BF16)]
    scratch += [vmem((4, width, W), BF16), vmem((4, width, W), BF16), vmem((4, W, width), BF16), dma((3,)), dma((4, 3))]
    flops = 34 * tokens * width * hidden
    return pl.pallas_call(
        functools.partial(train_kernel, plan),
        name="gradients",
        out_shape=(pltpu.VMEM((tiles, 3, 2 * half, LANES), BF16), jax.ShapeDtypeStruct((8, LANES), F32)),
        in_specs=[pl.BlockSpec(memory_space=pl.ANY)] * 5,
        out_specs=(pl.BlockSpec(memory_space=pltpu.VMEM), pl.BlockSpec(memory_space=pltpu.VMEM)),
        scratch_shapes=scratch,
        cost_estimate=pl.CostEstimate(flops=flops, bytes_accessed=12 * width * hidden * 2, transcendentals=0),
        compiler_params=pltpu.CompilerParams(collective_id=0, has_side_effects=True, vmem_limit_bytes=48_000_000),
    )(x, dy, *weights)


def adamw_kernel(count, squares_ref, g_ref, *refs):
    ws, ms, vs, new_ws, new_ms, new_vs = (refs[i : i + 3] for i in range(0, 18, 3))
    factor = jnp.minimum(1.0, 0.5 * lax.rsqrt(jnp.sum(squares_ref[...]) / count + 1e-30))
    step = pl.program_id(0)
    per, half, lines = g_ref.shape[0] // 2, g_ref.shape[2] // 2, ms[0].shape[1]
    first, at = div(step, per) * per, rem(step, per)

    def update(color, g, rows, columns):
        g = g.astype(F32) * factor
        m = 0.9 * ms[color][0, rows, columns] + 0.1 * g
        v = 0.95 * vs[color][0, rows, columns] + 0.05 * g * g
        w = ws[color][0, rows, columns].astype(F32)
        new_ws[color][0, rows, columns] = (w - 0.02 * (m * lax.rsqrt(v + 1e-8) + 0.1 * w)).astype(BF16)
        new_ms[color][0, rows, columns] = m
        new_vs[color][0, rows, columns] = v

    for color in range(2):
        for t in range(per):
            for block in range(2):
                g = g_ref[first + t, color, pl.ds(pl.multiple_of(block * half + at * lines, 8), lines), :]
                update(color, g, slice(None), pl.ds((2 * t + block) * LANES, LANES))
    for block in range(2):
        update(2, g_ref[step, 2, pl.ds(block * half, half), :].astype(F32).T, pl.ds(block * LANES, LANES), slice(None))


def adamw(g, squares, weights, m, v):
    tiles, half = g.shape[0], g.shape[2] // 2
    per = tiles // 2
    up = pl.BlockSpec((1, half // per, W * per), lambda i: (1 - i // per, i % per, 0))
    down = pl.BlockSpec((1, W, half), lambda i: (1 - i // per, i % per, 0))
    three = [up, up, down]
    out = [jax.ShapeDtypeStruct(a.shape, a.dtype) for a in (*weights, *m, *v)]
    return pl.pallas_call(
        functools.partial(adamw_kernel, float(sum(w.size for w in weights))),
        name="adamw",
        grid=(tiles,),
        out_shape=out,
        in_specs=[pl.BlockSpec(squares.shape, lambda i: (0, 0)), pl.BlockSpec(memory_space=pltpu.VMEM)] + three * 3,
        out_specs=three * 3,
        compiler_params=pltpu.CompilerParams(vmem_limit_bytes=48_000_000),
    )(squares, pltpu.with_memory_space_constraint(g, pltpu.VMEM), *weights, *m, *v)


def solution(mesh):
    plan = Plan((4, 4, 8), 16, 768)

    def step(x, dy, *arrays):
        weights, m, v = (arrays[i : i + 3] for i in (0, 3, 6))
        g, squares = gradients(plan, x, dy, weights)
        return tuple(adamw(g, squares, weights, m, v))

    return jax.shard_map(
        step,
        mesh=mesh,
        in_specs=(P(("rep", "dp"), None, None),) * 2 + (P(None, None, None),) * 9,
        out_specs=(P("rep", None, None),) * 9,
        check_vma=False,
    )
```

```python
import functools

import jax
import jax.numpy as jnp
from jax import lax
from jax.experimental import pallas as pl
from jax.experimental.pallas import tpu as pltpu
from jax.sharding import PartitionSpec as P

F32, BF16 = jnp.float32, jnp.bfloat16
MESH = pl.DeviceIdType.MESH
SLOTS = 5
W = 256
LANES = 128


def ring_steps(n):
    half = n // 2
    sums = [[(1, half + 1 - k, 0 if k > 1 else None)] + ([(-1, k - half - 1, 1 if k > 2 else None)] if k > 1 else []) for k in range(1, half + 1)]
    copies = [[(1, 1 - k)] + ([(-1, k - 1)] if k < half else []) for k in range(1, half + 1)]
    return sums, copies


class Plan:
    def __init__(self, sizes, tiles, half):
        self.sizes, self.tiles, self.half = sizes, tiles, half
        groups = [((0, (0, 1, 2)), (1, (1, 0, 2))), ((2, (2, 0, 1)),)]
        self.members, self.span, self.sums, self.copies = [], [], [], []
        self.length, self.chunk, self.piece, self.owners, self.keys = [], [], [], [], [(0, "core")]
        for members in groups:
            n1, n2, n3 = (sizes[a] for a in members[0][1])
            assert all(tuple(sizes[a] for a in axes) == (n1, n2, n3) for _, axes in members)
            sums, copies = ring_steps(n1)
            self.members.append(members)
            self.span.append((0, tiles))
            self.sums.append(sums)
            self.copies.append(copies)
            self.length.append((n1, n2, n3))
            self.chunk.append(half // n1)
            self.piece.append(half // (n1 * n2))
            self.owners.append(half // (n1 * n2) // 8)
            self.keys += [(len(self.span) - 1, f"{c}{k + 1}") for c in "ra" for k in range(len(sums))]
            self.keys += [(len(self.span) - 1, name) for name in ("p2", "p3", "b3", "b2", "out")]


def rem(a, b):
    return lax.rem(a, jnp.int32(b))


def div(a, b):
    return lax.div(a, jnp.int32(b))


def dot(a, b, dims=((1,), (0,))):
    return lax.dot_general(a, b, (dims, ((), ())), preferred_element_type=F32)


LAST = ((1,), (1,))


def normed(h):
    wide = h.astype(F32)
    return (wide * lax.rsqrt(jnp.mean(wide * wide, -1, keepdims=True) + 1e-6)).astype(BF16)


def train_kernel(plan, *refs):
    sizes, tiles, half = plan.sizes, plan.tiles, plan.half
    x_hbm, dy_hbm, gate_hbm, up_hbm, down_hbm = refs[:5]
    g, squares, down_all, a1_h, turned, p = refs[5:11]
    scratch = list(refs[11:])
    a1, h, at_, dt = a1_h.at[0], a1_h.at[1], turned.at[0], turned.at[1]

    def take(count):
        out, scratch[:] = scratch[:count], scratch[count:]
        return out

    mine, taken, s = take(3)
    ring_in, ring_out, pair_in, pair_out, kept, own_in, own_out, own_kept = (take(len(plan.span)) for _ in range(8))
    sq, = take(1)
    recv, send, sq_recv, sq_send_sem = take(4)
    d, a0, acc, dg, du, wg, wu, wd, in_sem, w_sem, keep_sem = take(11)
    tokens, width = d.shape
    per = tiles // 2
    rows = min(256, tokens)

    me = lax.axis_index("dp")
    core = rem(me, 2)
    at = [div(me, 2 * sizes[1] * sizes[2]), rem(div(me, 2 * sizes[2]), sizes[1]), rem(div(me, 2), sizes[2])]
    way = 1 - 2 * core

    def device(axis=None, place=None, other_core=False):
        c = [place if a == axis else at[a] for a in range(3)]
        return {"dp": ((c[0] * sizes[1] + c[1]) * sizes[2] + c[2]) * 2 + ((1 - core) if other_core else core)}

    def along(axis, step):
        return rem(at[axis] + step + 2 * sizes[axis], sizes[axis])


    def fetch(layer, t, slot, start, down=True):
        cols = pl.ds(pl.multiple_of(t * W, W), W)
        copies = [(gate_hbm.at[layer, :, cols], wg.at[slot]), (up_hbm.at[layer, :, cols], wu.at[slot])]
        if down:
            copies.append((down_hbm.at[layer, cols, :], wd.at[slot]))
        for i, (src, dst) in enumerate(copies):
            copy = pltpu.make_async_copy(src, dst, w_sem.at[slot, i])
            copy.start() if start else copy.wait()

    def fetch_tile(q, start):
        for layer in range(2):
            first = (1 - layer) * per

            @pl.when((q >= first) & (q < first + per))
            def _():
                fetch(layer, q - first, rem(q, 4), start)

    def tile_forward(slot, a, d):
        for r in range(0, tokens, rows):
            block = pl.ds(r, rows)
            gate = dot(a[block, :], wg[slot])
            up = dot(a[block, :], wu[slot])
            by_p = dot(d[block, :], wd[slot], LAST).astype(BF16).astype(F32)
            sig = jax.nn.sigmoid(gate)
            act = gate * sig
            p[block, 0:W] = (act * up).astype(BF16)
            du[block, :] = (by_p * act).astype(BF16)
            dg[block, :] = (by_p * up * (sig * (1 + gate * (1 - sig)))).astype(BF16)

    def tile_gradients(tile, dt):
        for color, (left, right) in enumerate(((at_, dg), (at_, du), (dt, p))):
            out = dot(left[...], right[:, 0:W])
            low, high = out[:, :LANES], out[:, LANES:]
            s[rem(tile, S_SLOTS), color] = jnp.where(core == 0, low, high)
            mine[rem(tile, 2), color] = jnp.where(core == 0, high, low).astype(BF16)

    def tile_by_input(slot):
        for r in range(0, tokens, rows):
            block = pl.ds(r, rows)
            acc[block, :] += dot(dg[block, :], wg[slot], LAST) + dot(du[block, :], wu[slot], LAST)

    def through_norm():
        for r in range(0, tokens, rows):
            block = pl.ds(r, rows)
            wide = h[block, :].astype(F32)
            scale = lax.rsqrt(jnp.mean(wide * wide, -1, keepdims=True) + 1e-6)
            by_a = acc[block, :].astype(BF16).astype(F32)
            by_h = by_a * scale - wide * (scale * scale * scale * (jnp.sum(by_a * wide, -1, keepdims=True) * (1.0 / width)))
            d[block, :] = (d[block, :].astype(F32) + by_h.astype(BF16).astype(F32)).astype(BF16)

    def forward():
        load_x = pltpu.make_async_copy(x_hbm.at[0], h, in_sem.at[0])
        load_dy = pltpu.make_async_copy(dy_hbm.at[0], d, in_sem.at[1])
        load_down = pltpu.make_async_copy(down_hbm.at[0], down_all, in_sem.at[2])
        load_x.start()
        for t in range(2):
            fetch(0, t, t, True, False)
        load_down.start()
        load_dy.start()
        load_x.wait()
        for r in range(0, tokens, rows):
            a0[r : r + rows, :] = normed(h[r : r + rows, :])

        def pair(i, carry):
            base = 2 * rem(i, 2)
            for k in range(2):
                fetch(0, 2 * i + k, base + k, False, False)

            @pl.when(i + 1 < per // 2)
            def _():
                for k in range(2):
                    fetch(0, 2 * i + 2 + k, 2 - base + k, True, False)

            @pl.when(i + 1 == per // 2)
            def _():
                fetch(1, 0, 2 - base, True)

            for k in range(2):
                for r in range(0, tokens, rows):
                    gate = dot(a0[r : r + rows, :], wg[base + k])
                    up = dot(a0[r : r + rows, :], wu[base + k])
                    p[r : r + rows, pl.ds(pl.multiple_of((2 * i + k) * W, W), W)] = (gate * jax.nn.sigmoid(gate) * up).astype(BF16)
            return carry

        lax.fori_loop(0, per // 2, pair, 0)
        load_down.wait()
        for r in range(0, tokens, rows):
            made = dot(p[r : r + rows, :], down_all[...]).astype(BF16).astype(F32)
            out = (h[r : r + rows, :].astype(F32) + made).astype(BF16)
            h[r : r + rows, :] = out
            a1[r : r + rows, :] = normed(out)
        at_[...] = a1[...].T
        acc[...] = jnp.zeros_like(acc)
        load_dy.wait()
        dt[...] = d[...].T
        fetch_tile(jnp.int32(0), False)
        fetch_tile(jnp.int32(1), True)
        tile_forward(0, a1, d)

    def gradients_of(tile):
        tile_gradients(tile, dt)

    def rest(tile):
        slot, after = rem(tile, 4), rem(tile + 1, 4)

        @pl.when(tile + 1 < tiles)
        def _():
            fetch_tile(tile + 1, False)

        @pl.when(tile + 2 < tiles)
        def _():
            fetch_tile(tile + 2, True)

        @pl.when(tile < per - 1)
        def _():
            tile_by_input(slot)
            tile_forward(after, a1, d)

        @pl.when(tile == per - 1)
        def _():
            tile_by_input(slot)
            through_norm()
            at_[...] = a0[...].T
            dt[...] = d[...].T
            tile_forward(after, a0, d)

        @pl.when((tile >= per) & (tile < tiles - 1))
        def _():
            tile_forward(after, a0, d)

    def weights_for_adamw(part):
        if down_all.shape[0] != 2 * tokens:
            return []
        if part == 0:
            pairs = [(down_hbm.at[1, pl.ds(k * tokens, tokens), :], a1_h.at[k]) for k in range(2)]
        else:
            pairs = [(gate_hbm.at[1, :, pl.ds(k * tokens, tokens)], turned.at[k]) for k in range(2)]
            pairs.append((up_hbm.at[1], p.at[pl.ds(0, width), :]))
        return [pltpu.make_async_copy(src, dst, keep_sem.at[2 * part + k]) for k, (src, dst) in enumerate(pairs)]


    def sem(array, group, stage, tile):
        return array.at[plan.keys.index((group, stage)), rem(tile, SLOTS)]

    def put(src, dst, group, stage, tile, where):
        pltpu.make_async_remote_copy(
            src_ref=src, dst_ref=dst, send_sem=sem(send, group, stage, tile), recv_sem=sem(recv, group, stage, tile),
            device_id=where, device_id_type=MESH,
        ).start()

    def wait(array, ref, group, stage, tile):
        pltpu.make_async_copy(ref, ref, sem(array, group, stage, tile)).wait()

    def some(group, tile, count):
        return g.at[tile, plan.members[group][0][0], pl.ds(0, count * len(plan.members[group])), :]

    def spot(weight, tile, row, count):
        return g.at[tile, weight, pl.ds(pl.multiple_of(row, 8), count), :]

    def eight(row, count):
        return pl.ds(pl.multiple_of(row, 8), count)

    def first_sends(group, tile, step):
        slot, out, chunk = rem(tile, R_SLOTS), rem(tile, 2), plan.chunk[group]
        for m, (weight, axes) in enumerate(plan.members[group]):
            for i, (to, whose, before) in enumerate(plan.sums[group][step - 1]):
                total = s[rem(tile, S_SLOTS), weight, eight(along(axes[0], way * whose) * chunk, chunk), :]
                if before is not None:
                    total += ring_in[group][slot, step - 2, before, m].astype(F32)
                ring_out[group][out, step - 1, i, m] = total.astype(BF16)
                put(ring_out[group].at[out, step - 1, i, m], ring_in[group].at[slot, step - 1, i, m], group, f"r{step}", tile,
                    device(axes[0], along(axes[0], way * to)))

    def first_wait(group, tile, step):
        count = len(plan.sums[group][step - 1])
        wait(recv, ring_in[group].at[rem(tile, R_SLOTS), step - 1, pl.ds(0, count)], group, f"r{step}", tile)
        wait(send, ring_out[group].at[rem(tile, 2), step - 1, pl.ds(0, count)], group, f"r{step}", tile)

    def first_next(group, tile, step):
        first_wait(group, tile, step - 1)
        first_sends(group, tile, step)

    def first_last(group, tile):
        steps, chunk, piece, slot = len(plan.sums[group]), plan.chunk[group], plan.piece[group], rem(tile, 2)
        first_wait(group, tile, steps)
        for m, (weight, axes) in enumerate(plan.members[group]):
            total = s[rem(tile, S_SLOTS), weight, eight(at[axes[0]] * chunk, chunk), :]
            for i in range(len(plan.sums[group][-1])):
                total += ring_in[group][rem(tile, R_SLOTS), steps - 1, i, m].astype(F32)
            kept[group][slot, m] = total
            for k in range(1, sizes[axes[1]]):
                owner = along(axes[1], k)
                pair_out[group][slot, k - 1, m] = kept[group][slot, m, eight(owner * piece, piece), :].astype(BF16)
                put(pair_out[group].at[slot, k - 1, m], pair_in[group].at[rem(tile, R_SLOTS), k - 1, m], group, "p2", tile, device(axes[1], owner))

    def exchanged(group, tile):
        piece, slot, n = plan.piece[group], rem(tile, SLOTS), plan.length[group][2]
        wait(recv, pair_in[group].at[rem(tile, R_SLOTS)], group, "p2", tile)
        wait(send, pair_out[group].at[rem(tile, 2)], group, "p2", tile)
        for m, (weight, axes) in enumerate(plan.members[group]):
            total = kept[group][rem(tile, 2), m, eight(at[axes[1]] * piece, piece), :]
            for k in range(1, sizes[axes[1]]):
                total += pair_in[group][rem(tile, R_SLOTS), k - 1, m].astype(F32)
            own_kept[group][slot, m] = total
            own_out[group][slot, m] = total.astype(BF16)
        last = plan.members[group][0][1][2]
        for owner in range(plan.owners[group]):

            @pl.when(at[last] != owner)
            def _():
                put(own_out[group].at[slot, :, pl.ds(8 * owner, 8)], own_in[group].at[slot, rem(at[last] + (n - 1 - owner), n)],
                    group, "p3", tile, device(last, jnp.int32(owner)))

    def place(group, axes):
        return core * half + at[axes[0]] * plan.chunk[group] + at[axes[1]] * plan.piece[group]

    def own_step(group, tile):
        n, slot, last = plan.length[group][2], rem(tile, SLOTS), plan.members[group][0][1][2]

        @pl.when(at[last] < plan.owners[group])
        def _():
            wait(recv, own_in[group].at[slot], group, "p3", tile)
            for m, (weight, axes) in enumerate(plan.members[group]):
                total = own_kept[group][slot, m, eight(8 * at[last], 8), :]
                for k in range(1, n):
                    total += own_in[group][slot, k - 1, m].astype(F32)
                final = total.astype(BF16)
                row = place(group, axes) + 8 * at[last]
                g[tile, weight, eight(row, 8), :] = final
                for k in range(1, n):
                    put(spot(weight, tile, row, 8), spot(weight, tile, row, 8), group, "b3", tile, device(last, along(last, k)))
                wide = final.astype(F32)
                mine_sq = sq.at[0, at[SQ_AXES[0]]]
                mine_sq[...] += wide * wide

        line_wait(send, group, tile, "p3")

    def line_wait(array, group, tile, stage):
        owners, last = plan.owners[group], plan.members[group][0][1][2]
        if owners > 1:

            @pl.when(at[last] < owners)
            def _():
                wait(array, some(group, tile, 8 * (owners - 1)), group, stage, tile)

        if owners < sizes[last]:

            @pl.when(at[last] >= owners)
            def _():
                wait(array, some(group, tile, 8 * owners), group, stage, tile)

    def spread(group, tile):
        last, piece = plan.members[group][0][1][2], plan.piece[group]

        @pl.when(at[last] < plan.owners[group])
        def _():
            wait(send, some(group, tile, (plan.length[group][2] - 1) * 8), group, "b3", tile)

        line_wait(recv, group, tile, "b3")
        for weight, axes in plan.members[group]:
            row = place(group, axes)
            for k in range(1, sizes[axes[1]]):
                put(spot(weight, tile, row, piece), spot(weight, tile, row, piece), group, "b2", tile, device(axes[1], along(axes[1], k)))

    def gather(group, tile, step):
        chunk = plan.chunk[group]
        if step == 1:
            for array in (recv, send):
                wait(array, some(group, tile, (plan.length[group][1] - 1) * plan.piece[group]), group, "b2", tile)
        else:
            gather_wait(group, tile, step - 1)
        for weight, axes in plan.members[group]:
            for to, whose in plan.copies[group][step - 1]:
                row = core * half + along(axes[0], way * whose) * chunk
                put(spot(weight, tile, row, chunk), spot(weight, tile, row, chunk), group, f"a{step}", tile, device(axes[0], along(axes[0], way * to)))

    def gather_wait(group, tile, step):
        for array in (recv, send):
            wait(array, some(group, tile, len(plan.copies[group][step - 1]) * plan.chunk[group]), group, f"a{step}", tile)

    def both(group):
        weights = [weight for weight, _ in plan.members[group]]
        return pl.ds(weights[0], len(weights))

    def gathered(group, tile):
        gather_wait(group, tile, len(plan.copies[group]))
        mine_half = g.at[tile, both(group), eight(core * half, half), :]
        put(mine_half, mine_half, group, "out", tile, device(other_core=True))

    def finish(group, tile):
        for array in (recv, send):
            wait(array, some(group, tile, half), group, "out", tile)

    def core_send(tile):
        put(mine.at[rem(tile, 2)], taken.at[rem(tile, 2)], 0, "core", tile, device(other_core=True))

    def core_take(tile):
        wait(recv, taken.at[rem(tile, 2)], 0, "core", tile)
        wait(send, taken.at[rem(tile, 2)], 0, "core", tile)
        for weight in range(3):
            s[rem(tile, S_SLOTS), weight] += taken[rem(tile, 2), weight].astype(F32)

    def sq_peers(level):
        if level == 3:
            return [(core, device(other_core=True))]
        axis = SQ_AXES[level]
        return [(at[axis], device(axis, along(axis, step))) for step in range(1, sizes[axis])]

    def sq_send(level):
        for index, peer in sq_peers(level):
            pltpu.make_async_remote_copy(
                src_ref=sq.at[level, index], dst_ref=sq.at[level, index], send_sem=sq_send_sem.at[level], recv_sem=sq_recv.at[level],
                device_id=peer, device_id_type=MESH,
            ).start()

    def sq_take(level):
        count = len(sq_peers(level))
        for array in (sq_recv, sq_send_sem):
            ref = sq.at[level, pl.ds(0, count)]
            pltpu.make_async_copy(ref, ref, array.at[level]).wait()
        total = sq[level, 0]
        for i in range(1, count + 1):
            total += sq[level, i]
        if level == 3:
            squares[...] = total
        else:
            sq[level + 1, (at[SQ_AXES[level + 1]] if level < 2 else core)] = total
            sq_send(level + 1)

    jobs = [(1, 0, 0, tiles, core_take)]
    for group in reversed(range(len(plan.span))):
        def add(delay, part, job, *rest, group=group):
            jobs.append((delay, part, *plan.span[group], lambda tile: job(group, tile, *rest)))

        steps = len(plan.sums[group])
        add(1, 0, first_sends, 1)
        for step in range(2, steps + 1):
            add(step, 0, first_next, step)
        add(steps + 1, 0, first_last)
        add(steps + 2, 0, exchanged)
        own = steps + (4 if plan.length[group][2] > 4 else 3)
        add(own, 0, own_step)
        own += 1 if plan.length[group][2] > 4 else 0
        add(own + 1, 1, spread)
        for step in range(1, steps + 1):
            add(own + 1 + step, 1, gather, step)
        add(own + 2 + steps, 1, gathered)
        add(own + 3 + steps, 1, finish)
    summed = max(job[0] + job[3] - tiles for job in jobs if job[1] == 0)
    jobs.append((summed, 0, tiles - 1, tiles, lambda tile: sq_send(0)))
    for level in range(4):
        jobs.append((summed + (2, 4, 6, 7)[level], 1, tiles - 1, tiles, lambda tile, level=level: sq_take(level)))
    jobs.sort(key=lambda job: job[0])
    ticks = max(job[0] + job[3] for job in jobs)

    peers = [device(other_core=True)]
    for axis in range(3):
        peers += [device(axis, along(axis, step)) for step in range(1, sizes[axis])]
    barrier = pltpu.get_barrier_semaphore()
    for peer in peers:
        pl.semaphore_signal(barrier, inc=1, device_id=peer, device_id_type=MESH)
    sq[...] = jnp.zeros_like(sq)
    forward()
    pl.semaphore_wait(barrier, len(peers))

    def run(now, some_jobs):
        for delay, _, first, end, job in some_jobs:
            tile = now - delay
            pl.when((tile >= first) & (tile < end))(functools.partial(job, tile))

    def tick(now, carry):
        for part in range(2):
            here = [job for job in jobs if job[1] == part]
            pl.when(now >= min(job[0] + job[2] for job in here))(functools.partial(run, now, here))

            @pl.when(now < tiles)
            def _():
                if part:
                    rest(now)
                    for k, when in enumerate((per, tiles - 1)):

                        @pl.when(now == when)
                        def _():
                            for copy in weights_for_adamw(k):
                                copy.start()

                else:
                    gradients_of(now)
                    core_send(now)
        return carry

    lax.fori_loop(0, ticks, tick, 0)
    for copy in weights_for_adamw(0) + weights_for_adamw(1):
        copy.wait()


S_SLOTS, R_SLOTS = 5, 4
SQ_AXES = (2, 1, 0)


def gradients(plan, x, dy, weights):
    tiles, half, chunk, piece = plan.tiles, plan.half, plan.chunk, plan.piece
    tokens, width = x.shape[1:]
    hidden = tiles // 2 * W
    vmem, dma = pltpu.VMEM, pltpu.SemaphoreType.DMA
    scratch = [
        vmem((2, 3, half, LANES), BF16),
        vmem((2, 3, half, LANES), BF16),
        vmem((S_SLOTS, 3, half, LANES), F32),
    ]
    groups = range(len(plan.span))
    count = [len(members) for members in plan.members]
    most = [max(len(step) for step in sums) for sums in plan.sums]
    scratch += [vmem((R_SLOTS, len(plan.sums[c]), most[c], count[c], chunk[c], LANES), BF16) for c in groups]
    scratch += [vmem((2, len(plan.sums[c]), most[c], count[c], chunk[c], LANES), BF16) for c in groups]
    scratch += [vmem((R_SLOTS, plan.length[c][1] - 1, count[c], piece[c], LANES), BF16) for c in groups]
    scratch += [vmem((2, plan.length[c][1] - 1, count[c], piece[c], LANES), BF16) for c in groups]
    scratch += [vmem((2, count[c], chunk[c], LANES), F32) for c in groups]
    scratch += [vmem((SLOTS, plan.length[c][2] - 1, count[c], 8, LANES), BF16) for c in groups]
    scratch += [vmem((SLOTS, count[c], piece[c], LANES), BF16) for c in groups]
    scratch += [vmem((SLOTS, count[c], piece[c], LANES), F32) for c in groups]
    scratch += [vmem((4, 8, 8, LANES), F32)]
    scratch += [dma((len(plan.keys), SLOTS)), dma((len(plan.keys), SLOTS)), dma((4,)), dma((4,))]
    scratch += [vmem((tokens, width), BF16), vmem((tokens, width), BF16), vmem((tokens, width), F32), vmem((tokens, W), BF16), vmem((tokens, W), BF16)]
    scratch += [vmem((4, width, W), BF16), vmem((4, width, W), BF16), vmem((4, W, width), BF16), dma((3,)), dma((4, 3)), dma((5,))]
    flops = 34 * tokens * width * hidden
    return pl.pallas_call(
        functools.partial(train_kernel, plan),
        name="gradients",
        out_shape=(
            vmem((tiles, 3, 2 * half, LANES), BF16), jax.ShapeDtypeStruct((8, LANES), F32), vmem((hidden, width), BF16),
            vmem((2, tokens, width), BF16), vmem((2, width, tokens), BF16), vmem((tokens, hidden), BF16),
        ),
        in_specs=[pl.BlockSpec(memory_space=pl.ANY)] * 5,
        out_specs=(pl.BlockSpec(memory_space=pltpu.VMEM),) * 6,
        scratch_shapes=scratch,
        cost_estimate=pl.CostEstimate(flops=flops, bytes_accessed=12 * width * hidden * 2, transcendentals=0),
        compiler_params=pltpu.CompilerParams(collective_id=0, has_side_effects=True, vmem_limit_bytes=34_400_000),
    )(x, dy, *weights)


def adamw_kernel(count, squares_ref, g_ref, down0, down1, gate1, up1, gate0, up0, *refs):
    ms, vs, new_ws, new_ms, new_vs = (refs[i : i + 3] for i in range(0, 15, 3))
    factor = jnp.minimum(1.0, 0.5 * lax.rsqrt(jnp.sum(squares_ref[...]) / count + 1e-30))
    step = pl.program_id(0)
    per, half, lines = g_ref.shape[0] // 2, g_ref.shape[2] // 2, ms[0].shape[1]
    at = rem(step, per)
    mine = pl.ds(pl.multiple_of(at * lines, 8), lines)

    def update(color, g, w, rows, columns):
        g, w = g.astype(F32) * factor, w.astype(F32)
        m = 0.9 * ms[color][0, rows, columns] + 0.1 * g
        v = 0.95 * vs[color][0, rows, columns] + 0.05 * g * g
        new_ws[color][0, rows, columns] = (w - 0.02 * (m * lax.rsqrt(v + 1e-8) + 0.1 * w)).astype(BF16)
        new_ms[color][0, rows, columns] = m
        new_vs[color][0, rows, columns] = v

    def layer(number):
        first, split, runs = (1 - number) * per, gate1.shape[2], down1.shape[1] // W
        for color in range(2):
            for t in range(per):
                for block in range(2):
                    g = g_ref[first + t, color, pl.ds(pl.multiple_of(block * half + at * lines, 8), lines), :]
                    column = (2 * t + block) * LANES
                    columns = pl.ds(column, LANES)
                    if number == 0:
                        w = (gate0, up0)[color][0, :, columns]
                    elif color == 0:
                        w = gate1[column // split, mine, pl.ds(column % split, LANES)]
                    else:
                        w = up1[mine, columns]
                    update(color, g, w, slice(None), columns)
        for block in range(2):
            g = g_ref[first + at, 2, pl.ds(block * half, half), :].astype(F32).T
            if number == 0:
                w = down0[pl.ds(pl.multiple_of(at * W + block * LANES, 8), LANES), :]
            else:
                w = down1[div(at, runs), pl.ds(pl.multiple_of(rem(at, runs) * W + block * LANES, 8), LANES), :]
            update(2, g, w, pl.ds(block * LANES, LANES), slice(None))

    pl.when(step < per)(functools.partial(layer, 1))
    pl.when(step >= per)(functools.partial(layer, 0))


def adamw(g, squares, kept, weights, m, v):
    tiles, half = g.shape[0], g.shape[2] // 2
    per = tiles // 2
    up = pl.BlockSpec((1, half // per, W * per), lambda i: (1 - i // per, i % per, 0))
    down = pl.BlockSpec((1, W, half), lambda i: (1 - i // per, i % per, 0))
    later = pl.BlockSpec((1, half // per, W * per), lambda i: (0, jnp.maximum(i - per, 0), 0))
    here = pl.BlockSpec(memory_space=pltpu.VMEM)
    out = [jax.ShapeDtypeStruct(a.shape, a.dtype) for a in (*weights, *m, *v)]
    in_vmem = [pltpu.with_memory_space_constraint(a, pltpu.VMEM) for a in (g, *kept)]
    return pl.pallas_call(
        functools.partial(adamw_kernel, float(sum(w.size for w in weights))),
        name="adamw",
        grid=(tiles,),
        out_shape=out,
        in_specs=[pl.BlockSpec(squares.shape, lambda i: (0, 0))] + [here] * 5 + [later] * 2 + [up, up, down] * 2,
        out_specs=[up, up, down] * 3,
        compiler_params=pltpu.CompilerParams(vmem_limit_bytes=34_400_000),
    )(squares, *in_vmem, *weights[:2], *m, *v)


def solution(mesh):
    plan = Plan((4, 4, 8), 16, 768)

    def step(x, dy, *arrays):
        weights, m, v = (arrays[i : i + 3] for i in (0, 3, 6))
        g, squares, *kept = gradients(plan, x, dy, weights)
        return tuple(adamw(g, squares, kept, weights, m, v))

    return jax.shard_map(
        step,
        mesh=mesh,
        in_specs=(P(("rep", "dp"), None, None),) * 2 + (P(None, None, None),) * 9,
        out_specs=(P("rep", None, None),) * 9,
        check_vma=False,
    )
```

```python
import functools

import jax
import jax.numpy as jnp
from jax import lax
from jax.experimental import pallas as pl
from jax.experimental.pallas import tpu as pltpu
from jax.sharding import PartitionSpec as P

F32, BF16 = jnp.float32, jnp.bfloat16
MESH = pl.DeviceIdType.MESH
SLOTS = 5
W = 256
LANES = 128


def ring_steps(n):
    half = n // 2
    sums = [[(1, half + 1 - k, 0 if k > 1 else None)] + ([(-1, k - half - 1, 1 if k > 2 else None)] if k > 1 else []) for k in range(1, half + 1)]
    copies = [[(1, 1 - k)] + ([(-1, k - 1)] if k < half else []) for k in range(1, half + 1)]
    return sums, copies


class Plan:
    def __init__(self, sizes, tiles, half):
        self.sizes, self.tiles, self.half = sizes, tiles, half
        groups = [((0, (0, 1, 2)), (1, (1, 0, 2))), ((2, (2, 0, 1)),)]
        self.members, self.span, self.sums, self.copies = [], [], [], []
        self.length, self.chunk, self.piece, self.owners, self.keys = [], [], [], [], [(0, "core")]
        for members in groups:
            n1, n2, n3 = (sizes[a] for a in members[0][1])
            assert all(tuple(sizes[a] for a in axes) == (n1, n2, n3) for _, axes in members)
            sums, copies = ring_steps(n1)
            self.members.append(members)
            self.span.append((0, tiles))
            self.sums.append(sums)
            self.copies.append(copies)
            self.length.append((n1, n2, n3))
            self.chunk.append(half // n1)
            self.piece.append(half // (n1 * n2))
            self.owners.append(half // (n1 * n2) // 8)
            self.keys += [(len(self.span) - 1, f"{c}{k + 1}") for c in "ra" for k in range(len(sums))]
            self.keys += [(len(self.span) - 1, name) for name in ("p2", "p3", "b3", "b2", "out")]


def rem(a, b):
    return lax.rem(a, jnp.int32(b))


def div(a, b):
    return lax.div(a, jnp.int32(b))


def dot(a, b, dims=((1,), (0,))):
    return lax.dot_general(a, b, (dims, ((), ())), preferred_element_type=F32)


LAST = ((1,), (1,))


def normed(h):
    wide = h.astype(F32)
    return (wide * lax.rsqrt(jnp.mean(wide * wide, -1, keepdims=True) + 1e-6)).astype(BF16)


def train_kernel(plan, *refs):
    sizes, tiles, half = plan.sizes, plan.tiles, plan.half
    x_hbm, dy_hbm, gate_hbm, up_hbm, down_hbm = refs[:5]
    g, squares = refs[5:7]
    scratch = list(refs[7:])

    def take(count):
        out, scratch[:] = scratch[:count], scratch[count:]
        return out

    mine, taken, s = take(3)
    ring_in, ring_out, pair_in, pair_out, kept, own_in, own_out, own_kept = (take(len(plan.span)) for _ in range(8))
    sq, = take(1)
    recv, send, sq_recv, sq_send_sem = take(4)
    h, d, a0, a1, at_, dt, acc, p, dg, du, down_all, wg, wu, wd, in_sem, w_sem = take(16)
    tokens, width = h.shape
    per = tiles // 2
    rows = min(256, tokens)

    me = lax.axis_index("dp")
    core = rem(me, 2)
    at = [div(me, 2 * sizes[1] * sizes[2]), rem(div(me, 2 * sizes[2]), sizes[1]), rem(div(me, 2), sizes[2])]
    way = 1 - 2 * core

    def device(axis=None, place=None, other_core=False):
        c = [place if a == axis else at[a] for a in range(3)]
        return {"dp": ((c[0] * sizes[1] + c[1]) * sizes[2] + c[2]) * 2 + ((1 - core) if other_core else core)}

    def along(axis, step):
        return rem(at[axis] + step + 2 * sizes[axis], sizes[axis])


    def fetch(layer, t, slot, start, down=True):
        cols = pl.ds(pl.multiple_of(t * W, W), W)
        copies = [(gate_hbm.at[layer, :, cols], wg.at[slot]), (up_hbm.at[layer, :, cols], wu.at[slot])]
        if down:
            copies.append((down_hbm.at[layer, cols, :], wd.at[slot]))
        for i, (src, dst) in enumerate(copies):
            copy = pltpu.make_async_copy(src, dst, w_sem.at[slot, i])
            copy.start() if start else copy.wait()

    def fetch_tile(q, start):
        for layer in range(2):
            first = (1 - layer) * per

            @pl.when((q >= first) & (q < first + per))
            def _():
                fetch(layer, q - first, rem(q, 4), start)

    def tile_forward(slot, a, d):
        for r in range(0, tokens, rows):
            block = pl.ds(r, rows)
            gate = dot(a[block, :], wg[slot])
            up = dot(a[block, :], wu[slot])
            by_p = dot(d[block, :], wd[slot], LAST).astype(BF16).astype(F32)
            sig = jax.nn.sigmoid(gate)
            act = gate * sig
            p[block, 0:W] = (act * up).astype(BF16)
            du[block, :] = (by_p * act).astype(BF16)
            dg[block, :] = (by_p * up * (sig * (1 + gate * (1 - sig)))).astype(BF16)

    def tile_gradients(tile, dt):
        for color, (left, right) in enumerate(((at_, dg), (at_, du), (dt, p))):
            out = dot(left[...], right[:, 0:W])
            low, high = out[:, :LANES], out[:, LANES:]
            s[rem(tile, S_SLOTS), color] = jnp.where(core == 0, low, high)
            mine[rem(tile, 2), color] = jnp.where(core == 0, high, low).astype(BF16)

    def tile_by_input(slot):
        for r in range(0, tokens, rows):
            block = pl.ds(r, rows)
            acc[block, :] += dot(dg[block, :], wg[slot], LAST) + dot(du[block, :], wu[slot], LAST)

    def through_norm():
        for r in range(0, tokens, rows):
            block = pl.ds(r, rows)
            wide = h[block, :].astype(F32)
            scale = lax.rsqrt(jnp.mean(wide * wide, -1, keepdims=True) + 1e-6)
            by_a = acc[block, :].astype(BF16).astype(F32)
            by_h = by_a * scale - wide * (scale * scale * scale * (jnp.sum(by_a * wide, -1, keepdims=True) * (1.0 / width)))
            d[block, :] = (d[block, :].astype(F32) + by_h.astype(BF16).astype(F32)).astype(BF16)

    def forward():
        load_x = pltpu.make_async_copy(x_hbm.at[0], h, in_sem.at[0])
        load_dy = pltpu.make_async_copy(dy_hbm.at[0], d, in_sem.at[1])
        load_down = pltpu.make_async_copy(down_hbm.at[0], down_all, in_sem.at[2])
        load_x.start()
        for t in range(2):
            fetch(0, t, t, True, False)
        load_down.start()
        load_dy.start()
        load_x.wait()
        for r in range(0, tokens, rows):
            a0[r : r + rows, :] = normed(h[r : r + rows, :])

        def pair(i, carry):
            base = 2 * rem(i, 2)
            for k in range(2):
                fetch(0, 2 * i + k, base + k, False, False)

            @pl.when(i + 1 < per // 2)
            def _():
                for k in range(2):
                    fetch(0, 2 * i + 2 + k, 2 - base + k, True, False)

            @pl.when(i + 1 == per // 2)
            def _():
                fetch(1, 0, 2 - base, True)

            for k in range(2):
                for r in range(0, tokens, rows):
                    gate = dot(a0[r : r + rows, :], wg[base + k])
                    up = dot(a0[r : r + rows, :], wu[base + k])
                    p[r : r + rows, pl.ds(pl.multiple_of((2 * i + k) * W, W), W)] = (gate * jax.nn.sigmoid(gate) * up).astype(BF16)
            return carry

        lax.fori_loop(0, per // 2, pair, 0)
        load_down.wait()
        for r in range(0, tokens, rows):
            made = dot(p[r : r + rows, :], down_all[...]).astype(BF16).astype(F32)
            out = (h[r : r + rows, :].astype(F32) + made).astype(BF16)
            h[r : r + rows, :] = out
            a1[r : r + rows, :] = normed(out)
        at_[...] = a1[...].T
        acc[...] = jnp.zeros_like(acc)
        load_dy.wait()
        dt[...] = d[...].T
        fetch_tile(jnp.int32(0), False)
        fetch_tile(jnp.int32(1), True)
        tile_forward(0, a1, d)

    def gradients_of(tile):
        tile_gradients(tile, dt)

    def rest(tile):
        slot, after = rem(tile, 4), rem(tile + 1, 4)

        @pl.when(tile + 1 < tiles)
        def _():
            fetch_tile(tile + 1, False)

        @pl.when(tile + 2 < tiles)
        def _():
            fetch_tile(tile + 2, True)

        @pl.when(tile < per - 1)
        def _():
            tile_by_input(slot)
            tile_forward(after, a1, d)

        @pl.when(tile == per - 1)
        def _():
            tile_by_input(slot)
            through_norm()
            at_[...] = a0[...].T
            dt[...] = d[...].T
            tile_forward(after, a0, d)

        @pl.when((tile >= per) & (tile < tiles - 1))
        def _():
            tile_forward(after, a0, d)


    def sem(array, group, stage, tile):
        return array.at[plan.keys.index((group, stage)), rem(tile, SLOTS)]

    def put(src, dst, group, stage, tile, where):
        pltpu.make_async_remote_copy(
            src_ref=src, dst_ref=dst, send_sem=sem(send, group, stage, tile), recv_sem=sem(recv, group, stage, tile),
            device_id=where, device_id_type=MESH,
        ).start()

    def wait(array, ref, group, stage, tile):
        pltpu.make_async_copy(ref, ref, sem(array, group, stage, tile)).wait()

    def some(group, tile, count):
        return g.at[tile, plan.members[group][0][0], pl.ds(0, count * len(plan.members[group])), :]

    def spot(weight, tile, row, count):
        return g.at[tile, weight, pl.ds(pl.multiple_of(row, 8), count), :]

    def eight(row, count):
        return pl.ds(pl.multiple_of(row, 8), count)

    def first_sends(group, tile, step):
        slot, out, chunk = rem(tile, R_SLOTS), rem(tile, 2), plan.chunk[group]
        for m, (weight, axes) in enumerate(plan.members[group]):
            for i, (to, whose, before) in enumerate(plan.sums[group][step - 1]):
                total = s[rem(tile, S_SLOTS), weight, eight(along(axes[0], way * whose) * chunk, chunk), :]
                if before is not None:
                    total += ring_in[group][slot, step - 2, before, m].astype(F32)
                ring_out[group][out, step - 1, i, m] = total.astype(BF16)
                put(ring_out[group].at[out, step - 1, i, m], ring_in[group].at[slot, step - 1, i, m], group, f"r{step}", tile,
                    device(axes[0], along(axes[0], way * to)))

    def first_wait(group, tile, step):
        count = len(plan.sums[group][step - 1])
        wait(recv, ring_in[group].at[rem(tile, R_SLOTS), step - 1, pl.ds(0, count)], group, f"r{step}", tile)
        wait(send, ring_out[group].at[rem(tile, 2), step - 1, pl.ds(0, count)], group, f"r{step}", tile)

    def first_next(group, tile, step):
        first_wait(group, tile, step - 1)
        first_sends(group, tile, step)

    def first_last(group, tile):
        steps, chunk, piece, slot = len(plan.sums[group]), plan.chunk[group], plan.piece[group], rem(tile, 2)
        first_wait(group, tile, steps)
        for m, (weight, axes) in enumerate(plan.members[group]):
            total = s[rem(tile, S_SLOTS), weight, eight(at[axes[0]] * chunk, chunk), :]
            for i in range(len(plan.sums[group][-1])):
                total += ring_in[group][rem(tile, R_SLOTS), steps - 1, i, m].astype(F32)
            kept[group][slot, m] = total
            for k in range(1, sizes[axes[1]]):
                owner = along(axes[1], k)
                pair_out[group][slot, k - 1, m] = kept[group][slot, m, eight(owner * piece, piece), :].astype(BF16)
                put(pair_out[group].at[slot, k - 1, m], pair_in[group].at[rem(tile, R_SLOTS), k - 1, m], group, "p2", tile, device(axes[1], owner))

    def exchanged(group, tile):
        piece, slot, n = plan.piece[group], rem(tile, SLOTS), plan.length[group][2]
        wait(recv, pair_in[group].at[rem(tile, R_SLOTS)], group, "p2", tile)
        wait(send, pair_out[group].at[rem(tile, 2)], group, "p2", tile)
        for m, (weight, axes) in enumerate(plan.members[group]):
            total = kept[group][rem(tile, 2), m, eight(at[axes[1]] * piece, piece), :]
            for k in range(1, sizes[axes[1]]):
                total += pair_in[group][rem(tile, R_SLOTS), k - 1, m].astype(F32)
            own_kept[group][slot, m] = total
            own_out[group][slot, m] = total.astype(BF16)
        last = plan.members[group][0][1][2]
        for owner in range(plan.owners[group]):

            @pl.when(at[last] != owner)
            def _():
                put(own_out[group].at[slot, :, pl.ds(8 * owner, 8)], own_in[group].at[slot, rem(at[last] + (n - 1 - owner), n)],
                    group, "p3", tile, device(last, jnp.int32(owner)))

    def place(group, axes):
        return core * half + at[axes[0]] * plan.chunk[group] + at[axes[1]] * plan.piece[group]

    def own_step(group, tile):
        n, slot, last = plan.length[group][2], rem(tile, SLOTS), plan.members[group][0][1][2]

        @pl.when(at[last] < plan.owners[group])
        def _():
            wait(recv, own_in[group].at[slot], group, "p3", tile)
            for m, (weight, axes) in enumerate(plan.members[group]):
                total = own_kept[group][slot, m, eight(8 * at[last], 8), :]
                for k in range(1, n):
                    total += own_in[group][slot, k - 1, m].astype(F32)
                final = total.astype(BF16)
                row = place(group, axes) + 8 * at[last]
                g[tile, weight, eight(row, 8), :] = final
                for k in range(1, n):
                    put(spot(weight, tile, row, 8), spot(weight, tile, row, 8), group, "b3", tile, device(last, along(last, k)))
                wide = final.astype(F32)
                mine_sq = sq.at[0, at[SQ_AXES[0]]]
                mine_sq[...] += wide * wide

        line_wait(send, group, tile, "p3")

    def line_wait(array, group, tile, stage):
        owners, last = plan.owners[group], plan.members[group][0][1][2]
        if owners > 1:

            @pl.when(at[last] < owners)
            def _():
                wait(array, some(group, tile, 8 * (owners - 1)), group, stage, tile)

        if owners < sizes[last]:

            @pl.when(at[last] >= owners)
            def _():
                wait(array, some(group, tile, 8 * owners), group, stage, tile)

    def spread(group, tile):
        last, piece = plan.members[group][0][1][2], plan.piece[group]

        @pl.when(at[last] < plan.owners[group])
        def _():
            wait(send, some(group, tile, (plan.length[group][2] - 1) * 8), group, "b3", tile)

        line_wait(recv, group, tile, "b3")
        for weight, axes in plan.members[group]:
            row = place(group, axes)
            for k in range(1, sizes[axes[1]]):
                put(spot(weight, tile, row, piece), spot(weight, tile, row, piece), group, "b2", tile, device(axes[1], along(axes[1], k)))

    def gather(group, tile, step):
        chunk = plan.chunk[group]
        if step == 1:
            for array in (recv, send):
                wait(array, some(group, tile, (plan.length[group][1] - 1) * plan.piece[group]), group, "b2", tile)
        else:
            gather_wait(group, tile, step - 1)
        for weight, axes in plan.members[group]:
            for to, whose in plan.copies[group][step - 1]:
                row = core * half + along(axes[0], way * whose) * chunk
                put(spot(weight, tile, row, chunk), spot(weight, tile, row, chunk), group, f"a{step}", tile, device(axes[0], along(axes[0], way * to)))

    def gather_wait(group, tile, step):
        for array in (recv, send):
            wait(array, some(group, tile, len(plan.copies[group][step - 1]) * plan.chunk[group]), group, f"a{step}", tile)

    def both(group):
        weights = [weight for weight, _ in plan.members[group]]
        return pl.ds(weights[0], len(weights))

    def gathered(group, tile):
        gather_wait(group, tile, len(plan.copies[group]))
        mine_half = g.at[tile, both(group), eight(core * half, half), :]
        put(mine_half, mine_half, group, "out", tile, device(other_core=True))

    def finish(group, tile):
        for array in (recv, send):
            wait(array, some(group, tile, half), group, "out", tile)

    def core_send(tile):
        put(mine.at[rem(tile, 2)], taken.at[rem(tile, 2)], 0, "core", tile, device(other_core=True))

    def core_take(tile):
        wait(recv, taken.at[rem(tile, 2)], 0, "core", tile)
        wait(send, taken.at[rem(tile, 2)], 0, "core", tile)
        for weight in range(3):
            s[rem(tile, S_SLOTS), weight] += taken[rem(tile, 2), weight].astype(F32)

    def sq_peers(level):
        if level == 3:
            return [(core, device(other_core=True))]
        axis = SQ_AXES[level]
        return [(at[axis], device(axis, along(axis, step))) for step in range(1, sizes[axis])]

    def sq_send(level):
        for index, peer in sq_peers(level):
            pltpu.make_async_remote_copy(
                src_ref=sq.at[level, index], dst_ref=sq.at[level, index], send_sem=sq_send_sem.at[level], recv_sem=sq_recv.at[level],
                device_id=peer, device_id_type=MESH,
            ).start()

    def sq_take(level):
        count = len(sq_peers(level))
        for array in (sq_recv, sq_send_sem):
            ref = sq.at[level, pl.ds(0, count)]
            pltpu.make_async_copy(ref, ref, array.at[level]).wait()
        total = sq[level, 0]
        for i in range(1, count + 1):
            total += sq[level, i]
        if level == 3:
            squares[...] = total
        else:
            sq[level + 1, (at[SQ_AXES[level + 1]] if level < 2 else core)] = total
            sq_send(level + 1)

    jobs = [(1, 0, 0, tiles, core_take)]
    for group in reversed(range(len(plan.span))):
        def add(delay, part, job, *rest, group=group):
            jobs.append((delay, part, *plan.span[group], lambda tile: job(group, tile, *rest)))

        steps = len(plan.sums[group])
        add(1, 0, first_sends, 1)
        for step in range(2, steps + 1):
            add(step, 0, first_next, step)
        add(steps + 1, 0, first_last)
        add(steps + 2, 0, exchanged)
        own = steps + (4 if plan.length[group][2] > 4 else 3)
        add(own, 0, own_step)
        own += 1 if plan.length[group][2] > 4 else 0
        add(own + 1, 1, spread)
        for step in range(1, steps + 1):
            add(own + 1 + step, 1, gather, step)
        add(own + 2 + steps, 1, gathered)
        add(own + 3 + steps, 1, finish)
    summed = max(job[0] + job[3] - tiles for job in jobs if job[1] == 0)
    jobs.append((summed, 0, tiles - 1, tiles, lambda tile: sq_send(0)))
    for level in range(4):
        jobs.append((summed + (2, 4, 6, 7)[level], 1, tiles - 1, tiles, lambda tile, level=level: sq_take(level)))
    jobs.sort(key=lambda job: job[0])
    ticks = max(job[0] + job[3] for job in jobs)

    peers = [device(other_core=True)]
    for axis in range(3):
        peers += [device(axis, along(axis, step)) for step in range(1, sizes[axis])]
    barrier = pltpu.get_barrier_semaphore()
    for peer in peers:
        pl.semaphore_signal(barrier, inc=1, device_id=peer, device_id_type=MESH)
    sq[...] = jnp.zeros_like(sq)
    forward()
    pl.semaphore_wait(barrier, len(peers))

    def run(now, some_jobs):
        for delay, _, first, end, job in some_jobs:
            tile = now - delay
            pl.when((tile >= first) & (tile < end))(functools.partial(job, tile))

    def tick(now, carry):
        for part in range(2):
            here = [job for job in jobs if job[1] == part]
            pl.when(now >= min(job[0] + job[2] for job in here))(functools.partial(run, now, here))

            @pl.when(now < tiles)
            def _():
                if part:
                    rest(now)
                else:
                    gradients_of(now)
                    core_send(now)
        return carry

    lax.fori_loop(0, ticks, tick, 0)


S_SLOTS, R_SLOTS = 5, 4
SQ_AXES = (2, 1, 0)


def gradients(plan, x, dy, weights):
    tiles, half, chunk, piece = plan.tiles, plan.half, plan.chunk, plan.piece
    tokens, width = x.shape[1:]
    hidden = tiles // 2 * W
    vmem, dma = pltpu.VMEM, pltpu.SemaphoreType.DMA
    scratch = [
        vmem((2, 3, half, LANES), BF16),
        vmem((2, 3, half, LANES), BF16),
        vmem((S_SLOTS, 3, half, LANES), F32),
    ]
    groups = range(len(plan.span))
    count = [len(members) for members in plan.members]
    most = [max(len(step) for step in sums) for sums in plan.sums]
    scratch += [vmem((R_SLOTS, len(plan.sums[c]), most[c], count[c], chunk[c], LANES), BF16) for c in groups]
    scratch += [vmem((2, len(plan.sums[c]), most[c], count[c], chunk[c], LANES), BF16) for c in groups]
    scratch += [vmem((R_SLOTS, plan.length[c][1] - 1, count[c], piece[c], LANES), BF16) for c in groups]
    scratch += [vmem((2, plan.length[c][1] - 1, count[c], piece[c], LANES), BF16) for c in groups]
    scratch += [vmem((2, count[c], chunk[c], LANES), F32) for c in groups]
    scratch += [vmem((SLOTS, plan.length[c][2] - 1, count[c], 8, LANES), BF16) for c in groups]
    scratch += [vmem((SLOTS, count[c], piece[c], LANES), BF16) for c in groups]
    scratch += [vmem((SLOTS, count[c], piece[c], LANES), F32) for c in groups]
    scratch += [vmem((4, 8, 8, LANES), F32)]
    scratch += [dma((len(plan.keys), SLOTS)), dma((len(plan.keys), SLOTS)), dma((4,)), dma((4,))]
    state, turned = vmem((tokens, width), BF16), vmem((width, tokens), BF16)
    scratch += [state, state, state, state, turned, turned, vmem((tokens, width), F32)]
    scratch += [vmem((tokens, hidden), BF16), vmem((tokens, W), BF16), vmem((tokens, W), BF16), vmem((hidden, width), BF16)]
    scratch += [vmem((4, width, W), BF16), vmem((4, width, W), BF16), vmem((4, W, width), BF16), dma((3,)), dma((4, 3))]
    flops = 34 * tokens * width * hidden
    return pl.pallas_call(
        functools.partial(train_kernel, plan),
        name="gradients",
        out_shape=(pltpu.VMEM((tiles, 3, 2 * half, LANES), BF16), jax.ShapeDtypeStruct((8, LANES), F32)),
        in_specs=[pl.BlockSpec(memory_space=pl.ANY)] * 5,
        out_specs=(pl.BlockSpec(memory_space=pltpu.VMEM), pl.BlockSpec(memory_space=pltpu.VMEM)),
        scratch_shapes=scratch,
        cost_estimate=pl.CostEstimate(flops=flops, bytes_accessed=12 * width * hidden * 2, transcendentals=0),
        compiler_params=pltpu.CompilerParams(collective_id=0, has_side_effects=True, vmem_limit_bytes=48_000_000),
    )(x, dy, *weights)


def adamw_kernel(count, squares_ref, g_ref, *refs):
    ws, ms, vs, new_ws, new_ms, new_vs = (refs[i : i + 3] for i in range(0, 18, 3))
    factor = jnp.minimum(1.0, 0.5 * lax.rsqrt(jnp.sum(squares_ref[...]) / count + 1e-30))
    step = pl.program_id(0)
    per, half, lines = g_ref.shape[0] // 2, g_ref.shape[2] // 2, ms[0].shape[1]
    first, at = div(step, per) * per, rem(step, per)

    def update(color, g, rows, columns):
        g = g.astype(F32) * factor
        m = 0.9 * ms[color][0, rows, columns] + 0.1 * g
        v = 0.95 * vs[color][0, rows, columns] + 0.05 * g * g
        w = ws[color][0, rows, columns].astype(F32)
        new_ws[color][0, rows, columns] = (w - 0.02 * (m * lax.rsqrt(v + 1e-8) + 0.1 * w)).astype(BF16)
        new_ms[color][0, rows, columns] = m
        new_vs[color][0, rows, columns] = v

    for color in range(2):
        for t in range(per):
            for block in range(2):
                g = g_ref[first + t, color, pl.ds(pl.multiple_of(block * half + at * lines, 8), lines), :]
                update(color, g, slice(None), pl.ds((2 * t + block) * LANES, LANES))
    for block in range(2):
        update(2, g_ref[step, 2, pl.ds(block * half, half), :].astype(F32).T, pl.ds(block * LANES, LANES), slice(None))


def adamw(g, squares, weights, m, v):
    tiles, half = g.shape[0], g.shape[2] // 2
    per = tiles // 2
    up = pl.BlockSpec((1, half // per, W * per), lambda i: (1 - i // per, i % per, 0))
    down = pl.BlockSpec((1, W, half), lambda i: (1 - i // per, i % per, 0))
    three = [up, up, down]
    out = [jax.ShapeDtypeStruct(a.shape, a.dtype) for a in (*weights, *m, *v)]
    return pl.pallas_call(
        functools.partial(adamw_kernel, float(sum(w.size for w in weights))),
        name="adamw",
        grid=(tiles,),
        out_shape=out,
        in_specs=[pl.BlockSpec(squares.shape, lambda i: (0, 0)), pl.BlockSpec(memory_space=pltpu.VMEM)] + three * 3,
        out_specs=three * 3,
        compiler_params=pltpu.CompilerParams(vmem_limit_bytes=48_000_000),
    )(squares, pltpu.with_memory_space_constraint(g, pltpu.VMEM), *weights, *m, *v)


def solution(mesh):
    plan = Plan((4, 4, 8), 16, 768)

    def step(x, dy, *arrays):
        weights, m, v = (arrays[i : i + 3] for i in (0, 3, 6))
        g, squares = gradients(plan, x, dy, weights)
        return tuple(adamw(g, squares, weights, m, v))

    return jax.shard_map(
        step,
        mesh=mesh,
        in_specs=(P(("rep", "dp"), None, None),) * 2 + (P(None, None, None),) * 9,
        out_specs=(P("rep", None, None),) * 9,
        check_vma=False,
    )
```

```python
import functools

import jax
import jax.numpy as jnp
from jax import lax
from jax.experimental import pallas as pl
from jax.experimental.pallas import tpu as pltpu
from jax.sharding import PartitionSpec as P

F32, BF16 = jnp.float32, jnp.bfloat16
MESH = pl.DeviceIdType.MESH
SLOTS = 5
W = 256
LANES = 128


def ring_steps(n):
    half = n // 2
    sums = [[(1, half + 1 - k, 0 if k > 1 else None)] + ([(-1, k - half - 1, 1 if k > 2 else None)] if k > 1 else []) for k in range(1, half + 1)]
    copies = [[(1, 1 - k)] + ([(-1, k - 1)] if k < half else []) for k in range(1, half + 1)]
    return sums, copies


class Plan:
    def __init__(self, sizes, tiles, half):
        self.sizes, self.tiles, self.half = sizes, tiles, half
        groups = [((0, (0, 1, 2)), (1, (1, 0, 2))), ((2, (2, 0, 1)),)]
        self.members, self.span, self.sums, self.copies = [], [], [], []
        self.length, self.chunk, self.piece, self.owners, self.keys = [], [], [], [], [(0, "core")]
        for members in groups:
            n1, n2, n3 = (sizes[a] for a in members[0][1])
            assert all(tuple(sizes[a] for a in axes) == (n1, n2, n3) for _, axes in members)
            sums, copies = ring_steps(n1)
            self.members.append(members)
            self.span.append((0, tiles))
            self.sums.append(sums)
            self.copies.append(copies)
            self.length.append((n1, n2, n3))
            self.chunk.append(half // n1)
            self.piece.append(half // (n1 * n2))
            self.owners.append(half // (n1 * n2) // 8)
            self.keys += [(len(self.span) - 1, f"{c}{k + 1}") for c in "ra" for k in range(len(sums))]
            self.keys += [(len(self.span) - 1, name) for name in ("p2", "p3", "b3", "b2", "out")]


def rem(a, b):
    return lax.rem(a, jnp.int32(b))


def div(a, b):
    return lax.div(a, jnp.int32(b))


def dot(a, b, dims=((1,), (0,))):
    return lax.dot_general(a, b, (dims, ((), ())), preferred_element_type=F32)


LAST = ((1,), (1,))


def normed(h):
    wide = h.astype(F32)
    return (wide * lax.rsqrt(jnp.mean(wide * wide, -1, keepdims=True) + 1e-6)).astype(BF16)


def train_kernel(plan, *refs):
    sizes, tiles, half = plan.sizes, plan.tiles, plan.half
    x_hbm, dy_hbm, gate_hbm, up_hbm, down_hbm = refs[:5]
    g, squares = refs[5:7]
    scratch = list(refs[7:])

    def take(count):
        out, scratch[:] = scratch[:count], scratch[count:]
        return out

    mine, taken, s = take(3)
    ring_in, ring_out, pair_in, pair_out, kept, own_in, own_out, own_kept = (take(len(plan.span)) for _ in range(8))
    sq, = take(1)
    recv, send, sq_recv, sq_send_sem = take(4)
    h, d, a0, a1, at_, dt, acc, p, dg, du, down_all, wg, wu, wd, in_sem, w_sem = take(16)
    tokens, width = h.shape
    per = tiles // 2
    rows = min(256, tokens)

    me = lax.axis_index("dp")
    core = rem(me, 2)
    at = [div(me, 2 * sizes[1] * sizes[2]), rem(div(me, 2 * sizes[2]), sizes[1]), rem(div(me, 2), sizes[2])]
    way = 1 - 2 * core

    def device(axis=None, place=None, other_core=False):
        c = [place if a == axis else at[a] for a in range(3)]
        return {"dp": ((c[0] * sizes[1] + c[1]) * sizes[2] + c[2]) * 2 + ((1 - core) if other_core else core)}

    def along(axis, step):
        return rem(at[axis] + step + 2 * sizes[axis], sizes[axis])


    def fetch(layer, t, slot, start, down=True):
        cols = pl.ds(pl.multiple_of(t * W, W), W)
        copies = [(gate_hbm.at[layer, :, cols], wg.at[slot]), (up_hbm.at[layer, :, cols], wu.at[slot])]
        if down:
            copies.append((down_hbm.at[layer, cols, :], wd.at[slot]))
        for i, (src, dst) in enumerate(copies):
            copy = pltpu.make_async_copy(src, dst, w_sem.at[slot, i])
            copy.start() if start else copy.wait()

    def fetch_tile(q, start):
        for layer in range(2):
            first = (1 - layer) * per

            @pl.when((q >= first) & (q < first + per))
            def _():
                fetch(layer, q - first, rem(q, 4), start)

    def tile_forward(slot, a, d):
        for r in range(0, tokens, rows):
            block = pl.ds(r, rows)
            gate = dot(a[block, :], wg[slot])
            up = dot(a[block, :], wu[slot])
            by_p = dot(d[block, :], wd[slot], LAST).astype(BF16).astype(F32)
            sig = jax.nn.sigmoid(gate)
            act = gate * sig
            p[block, 0:W] = (act * up).astype(BF16)
            du[block, :] = (by_p * act).astype(BF16)
            dg[block, :] = (by_p * up * (sig * (1 + gate * (1 - sig)))).astype(BF16)

    def tile_gradients(tile, dt):
        for color, (left, right) in enumerate(((at_, dg), (at_, du), (dt, p))):
            out = dot(left[...], right[:, 0:W])
            low, high = out[:, :LANES], out[:, LANES:]
            s[rem(tile, S_SLOTS), color] = jnp.where(core == 0, low, high)
            mine[rem(tile, 2), color] = jnp.where(core == 0, high, low).astype(BF16)

    def tile_by_input(slot):
        for r in range(0, tokens, rows):
            block = pl.ds(r, rows)
            acc[block, :] += dot(dg[block, :], wg[slot], LAST) + dot(du[block, :], wu[slot], LAST)

    def through_norm():
        for r in range(0, tokens, rows):
            block = pl.ds(r, rows)
            wide = h[block, :].astype(F32)
            scale = lax.rsqrt(jnp.mean(wide * wide, -1, keepdims=True) + 1e-6)
            by_a = acc[block, :].astype(BF16).astype(F32)
            by_h = by_a * scale - wide * (scale * scale * scale * (jnp.sum(by_a * wide, -1, keepdims=True) * (1.0 / width)))
            d[block, :] = (d[block, :].astype(F32) + by_h.astype(BF16).astype(F32)).astype(BF16)

    def forward():
        load_x = [
            pltpu.make_async_copy(x_hbm.at[0, pl.ds(r, rows), :], h.at[pl.ds(r, rows), :], in_sem.at[3 + r // rows]) for r in range(0, tokens, rows)
        ]
        load_dy = pltpu.make_async_copy(dy_hbm.at[0], d, in_sem.at[1])
        load_down = pltpu.make_async_copy(down_hbm.at[0], down_all, in_sem.at[2])
        for copy in load_x:
            copy.start()
        for t in range(2):
            fetch(0, t, t, True, False)
        for r in range(0, tokens, rows):
            load_x[r // rows].wait()
            a0[r : r + rows, :] = normed(h[r : r + rows, :])
        load_down.start()
        load_dy.start()

        def pair(i, carry):
            base = 2 * rem(i, 2)
            for k in range(2):
                fetch(0, 2 * i + k, base + k, False, False)

            @pl.when(i + 1 < per // 2)
            def _():
                for k in range(2):
                    fetch(0, 2 * i + 2 + k, 2 - base + k, True, False)

            @pl.when(i + 1 == per // 2)
            def _():
                fetch(1, 0, 2 - base, True)

            for k in range(2):
                for r in range(0, tokens, rows):
                    gate = dot(a0[r : r + rows, :], wg[base + k])
                    up = dot(a0[r : r + rows, :], wu[base + k])
                    p[r : r + rows, pl.ds(pl.multiple_of((2 * i + k) * W, W), W)] = (gate * jax.nn.sigmoid(gate) * up).astype(BF16)
            return carry

        lax.fori_loop(0, per // 2, pair, 0)
        load_down.wait()
        for r in range(0, tokens, rows):
            made = dot(p[r : r + rows, :], down_all[...]).astype(BF16).astype(F32)
            out = (h[r : r + rows, :].astype(F32) + made).astype(BF16)
            h[r : r + rows, :] = out
            a1[r : r + rows, :] = normed(out)
        at_[...] = a1[...].T
        acc[...] = jnp.zeros_like(acc)
        load_dy.wait()
        dt[...] = d[...].T
        fetch_tile(jnp.int32(0), False)
        fetch_tile(jnp.int32(1), True)
        tile_forward(0, a1, d)

    def gradients_of(tile):
        tile_gradients(tile, dt)

    def rest(tile):
        slot, after = rem(tile, 4), rem(tile + 1, 4)

        @pl.when(tile + 1 < tiles)
        def _():
            fetch_tile(tile + 1, False)

        @pl.when(tile + 2 < tiles)
        def _():
            fetch_tile(tile + 2, True)

        @pl.when(tile < per - 1)
        def _():
            tile_by_input(slot)
            tile_forward(after, a1, d)

        @pl.when(tile == per - 1)
        def _():
            tile_by_input(slot)
            through_norm()
            at_[...] = a0[...].T
            dt[...] = d[...].T
            tile_forward(after, a0, d)

        @pl.when((tile >= per) & (tile < tiles - 1))
        def _():
            tile_forward(after, a0, d)


    def sem(array, group, stage, tile):
        return array.at[plan.keys.index((group, stage)), rem(tile, SLOTS)]

    def put(src, dst, group, stage, tile, where):
        pltpu.make_async_remote_copy(
            src_ref=src, dst_ref=dst, send_sem=sem(send, group, stage, tile), recv_sem=sem(recv, group, stage, tile),
            device_id=where, device_id_type=MESH,
        ).start()

    def wait(array, ref, group, stage, tile):
        pltpu.make_async_copy(ref, ref, sem(array, group, stage, tile)).wait()

    def some(group, tile, count):
        return g.at[tile, plan.members[group][0][0], pl.ds(0, count * len(plan.members[group])), :]

    def spot(weight, tile, row, count):
        return g.at[tile, weight, pl.ds(pl.multiple_of(row, 8), count), :]

    def eight(row, count):
        return pl.ds(pl.multiple_of(row, 8), count)

    def first_sends(group, tile, step):
        slot, out, chunk = rem(tile, R_SLOTS), rem(tile, 2), plan.chunk[group]
        for m, (weight, axes) in enumerate(plan.members[group]):
            for i, (to, whose, before) in enumerate(plan.sums[group][step - 1]):
                total = s[rem(tile, S_SLOTS), weight, eight(along(axes[0], way * whose) * chunk, chunk), :]
                if before is not None:
                    total += ring_in[group][slot, step - 2, before, m].astype(F32)
                ring_out[group][out, step - 1, i, m] = total.astype(BF16)
                put(ring_out[group].at[out, step - 1, i, m], ring_in[group].at[slot, step - 1, i, m], group, f"r{step}", tile,
                    device(axes[0], along(axes[0], way * to)))

    def first_wait(group, tile, step):
        count = len(plan.sums[group][step - 1])
        wait(recv, ring_in[group].at[rem(tile, R_SLOTS), step - 1, pl.ds(0, count)], group, f"r{step}", tile)
        wait(send, ring_out[group].at[rem(tile, 2), step - 1, pl.ds(0, count)], group, f"r{step}", tile)

    def first_next(group, tile, step):
        first_wait(group, tile, step - 1)
        first_sends(group, tile, step)

    def first_last(group, tile):
        steps, chunk, piece, slot = len(plan.sums[group]), plan.chunk[group], plan.piece[group], rem(tile, 2)
        first_wait(group, tile, steps)
        for m, (weight, axes) in enumerate(plan.members[group]):
            total = s[rem(tile, S_SLOTS), weight, eight(at[axes[0]] * chunk, chunk), :]
            for i in range(len(plan.sums[group][-1])):
                total += ring_in[group][rem(tile, R_SLOTS), steps - 1, i, m].astype(F32)
            kept[group][slot, m] = total
            for k in range(1, sizes[axes[1]]):
                owner = along(axes[1], k)
                pair_out[group][slot, k - 1, m] = kept[group][slot, m, eight(owner * piece, piece), :].astype(BF16)
                put(pair_out[group].at[slot, k - 1, m], pair_in[group].at[rem(tile, R_SLOTS), k - 1, m], group, "p2", tile, device(axes[1], owner))

    def exchanged(group, tile):
        piece, slot, n = plan.piece[group], rem(tile, SLOTS), plan.length[group][2]
        wait(recv, pair_in[group].at[rem(tile, R_SLOTS)], group, "p2", tile)
        wait(send, pair_out[group].at[rem(tile, 2)], group, "p2", tile)
        for m, (weight, axes) in enumerate(plan.members[group]):
            total = kept[group][rem(tile, 2), m, eight(at[axes[1]] * piece, piece), :]
            for k in range(1, sizes[axes[1]]):
                total += pair_in[group][rem(tile, R_SLOTS), k - 1, m].astype(F32)
            own_kept[group][slot, m] = total
            own_out[group][slot, m] = total.astype(BF16)
        last = plan.members[group][0][1][2]
        for owner in range(plan.owners[group]):

            @pl.when(at[last] != owner)
            def _():
                put(own_out[group].at[slot, :, pl.ds(8 * owner, 8)], own_in[group].at[slot, rem(at[last] + (n - 1 - owner), n)],
                    group, "p3", tile, device(last, jnp.int32(owner)))

    def place(group, axes):
        return core * half + at[axes[0]] * plan.chunk[group] + at[axes[1]] * plan.piece[group]

    def own_step(group, tile):
        n, slot, last = plan.length[group][2], rem(tile, SLOTS), plan.members[group][0][1][2]

        @pl.when(at[last] < plan.owners[group])
        def _():
            wait(recv, own_in[group].at[slot], group, "p3", tile)
            for m, (weight, axes) in enumerate(plan.members[group]):
                total = own_kept[group][slot, m, eight(8 * at[last], 8), :]
                for k in range(1, n):
                    total += own_in[group][slot, k - 1, m].astype(F32)
                final = total.astype(BF16)
                row = place(group, axes) + 8 * at[last]
                g[tile, weight, eight(row, 8), :] = final
                for k in range(1, n):
                    put(spot(weight, tile, row, 8), spot(weight, tile, row, 8), group, "b3", tile, device(last, along(last, k)))
                wide = final.astype(F32)
                mine_sq = sq.at[0, at[SQ_AXES[0]]]
                mine_sq[...] += wide * wide

        line_wait(send, group, tile, "p3")

    def line_wait(array, group, tile, stage):
        owners, last = plan.owners[group], plan.members[group][0][1][2]
        if owners > 1:

            @pl.when(at[last] < owners)
            def _():
                wait(array, some(group, tile, 8 * (owners - 1)), group, stage, tile)

        if owners < sizes[last]:

            @pl.when(at[last] >= owners)
            def _():
                wait(array, some(group, tile, 8 * owners), group, stage, tile)

    def spread(group, tile):
        last, piece = plan.members[group][0][1][2], plan.piece[group]

        @pl.when(at[last] < plan.owners[group])
        def _():
            wait(send, some(group, tile, (plan.length[group][2] - 1) * 8), group, "b3", tile)

        line_wait(recv, group, tile, "b3")
        for weight, axes in plan.members[group]:
            row = place(group, axes)
            for k in range(1, sizes[axes[1]]):
                put(spot(weight, tile, row, piece), spot(weight, tile, row, piece), group, "b2", tile, device(axes[1], along(axes[1], k)))

    def gather(group, tile, step):
        chunk = plan.chunk[group]
        if step == 1:
            for array in (recv, send):
                wait(array, some(group, tile, (plan.length[group][1] - 1) * plan.piece[group]), group, "b2", tile)
        else:
            gather_wait(group, tile, step - 1)
        for weight, axes in plan.members[group]:
            for to, whose in plan.copies[group][step - 1]:
                row = core * half + along(axes[0], way * whose) * chunk
                put(spot(weight, tile, row, chunk), spot(weight, tile, row, chunk), group, f"a{step}", tile, device(axes[0], along(axes[0], way * to)))

    def gather_wait(group, tile, step):
        for array in (recv, send):
            wait(array, some(group, tile, len(plan.copies[group][step - 1]) * plan.chunk[group]), group, f"a{step}", tile)

    def both(group):
        weights = [weight for weight, _ in plan.members[group]]
        return pl.ds(weights[0], len(weights))

    def gathered(group, tile):
        gather_wait(group, tile, len(plan.copies[group]))
        mine_half = g.at[tile, both(group), eight(core * half, half), :]
        put(mine_half, mine_half, group, "out", tile, device(other_core=True))

    def finish(group, tile):
        for array in (recv, send):
            wait(array, some(group, tile, half), group, "out", tile)

    def core_send(tile):
        put(mine.at[rem(tile, 2)], taken.at[rem(tile, 2)], 0, "core", tile, device(other_core=True))

    def core_take(tile):
        wait(recv, taken.at[rem(tile, 2)], 0, "core", tile)
        wait(send, taken.at[rem(tile, 2)], 0, "core", tile)
        for weight in range(3):
            s[rem(tile, S_SLOTS), weight] += taken[rem(tile, 2), weight].astype(F32)

    def sq_peers(level):
        if level == 3:
            return [(core, device(other_core=True))]
        axis = SQ_AXES[level]
        return [(at[axis], device(axis, along(axis, step))) for step in range(1, sizes[axis])]

    def sq_send(level):
        for index, peer in sq_peers(level):
            pltpu.make_async_remote_copy(
                src_ref=sq.at[level, index], dst_ref=sq.at[level, index], send_sem=sq_send_sem.at[level], recv_sem=sq_recv.at[level],
                device_id=peer, device_id_type=MESH,
            ).start()

    def sq_take(level):
        count = len(sq_peers(level))
        for array in (sq_recv, sq_send_sem):
            ref = sq.at[level, pl.ds(0, count)]
            pltpu.make_async_copy(ref, ref, array.at[level]).wait()
        total = sq[level, 0]
        for i in range(1, count + 1):
            total += sq[level, i]
        if level == 3:
            squares[...] = total
        else:
            sq[level + 1, (at[SQ_AXES[level + 1]] if level < 2 else core)] = total
            sq_send(level + 1)

    jobs = [(1, 0, 0, tiles, core_take)]
    for group in reversed(range(len(plan.span))):
        def add(delay, part, job, *rest, group=group):
            jobs.append((delay, part, *plan.span[group], lambda tile: job(group, tile, *rest)))

        steps = len(plan.sums[group])
        add(1, 0, first_sends, 1)
        for step in range(2, steps + 1):
            add(step, 0, first_next, step)
        add(steps + 1, 0, first_last)
        add(steps + 2, 0, exchanged)
        own = steps + (4 if plan.length[group][2] > 4 else 3)
        add(own, 0, own_step)
        own += 1 if plan.length[group][2] > 4 else 0
        add(own + 1, 1, spread)
        for step in range(1, steps + 1):
            add(own + 1 + step, 1, gather, step)
        add(own + 2 + steps, 1, gathered)
        add(own + 3 + steps, 1, finish)
    summed = max(job[0] + job[3] - tiles for job in jobs if job[1] == 0)
    jobs.append((summed, 0, tiles - 1, tiles, lambda tile: sq_send(0)))
    for level in range(4):
        jobs.append((summed + (2, 4, 6, 7)[level], 1, tiles - 1, tiles, lambda tile, level=level: sq_take(level)))
    jobs.sort(key=lambda job: job[0])
    ticks = max(job[0] + job[3] for job in jobs)

    peers = [device(other_core=True)]
    for axis in range(3):
        peers += [device(axis, along(axis, step)) for step in range(1, sizes[axis])]
    barrier = pltpu.get_barrier_semaphore()
    for peer in peers:
        pl.semaphore_signal(barrier, inc=1, device_id=peer, device_id_type=MESH)
    sq[...] = jnp.zeros_like(sq)
    forward()
    pl.semaphore_wait(barrier, len(peers))

    def run(now, some_jobs):
        for delay, _, first, end, job in some_jobs:
            tile = now - delay
            pl.when((tile >= first) & (tile < end))(functools.partial(job, tile))

    def tick(now, carry):
        for part in range(2):
            here = [job for job in jobs if job[1] == part]
            pl.when(now >= min(job[0] + job[2] for job in here))(functools.partial(run, now, here))

            @pl.when(now < tiles)
            def _():
                if part:
                    rest(now)
                else:
                    gradients_of(now)
                    core_send(now)
        return carry

    lax.fori_loop(0, ticks, tick, 0)


S_SLOTS, R_SLOTS = 5, 4
SQ_AXES = (2, 1, 0)


def gradients(plan, x, dy, weights):
    tiles, half, chunk, piece = plan.tiles, plan.half, plan.chunk, plan.piece
    tokens, width = x.shape[1:]
    hidden = tiles // 2 * W
    vmem, dma = pltpu.VMEM, pltpu.SemaphoreType.DMA
    scratch = [
        vmem((2, 3, half, LANES), BF16),
        vmem((2, 3, half, LANES), BF16),
        vmem((S_SLOTS, 3, half, LANES), F32),
    ]
    groups = range(len(plan.span))
    count = [len(members) for members in plan.members]
    most = [max(len(step) for step in sums) for sums in plan.sums]
    scratch += [vmem((R_SLOTS, len(plan.sums[c]), most[c], count[c], chunk[c], LANES), BF16) for c in groups]
    scratch += [vmem((2, len(plan.sums[c]), most[c], count[c], chunk[c], LANES), BF16) for c in groups]
    scratch += [vmem((R_SLOTS, plan.length[c][1] - 1, count[c], piece[c], LANES), BF16) for c in groups]
    scratch += [vmem((2, plan.length[c][1] - 1, count[c], piece[c], LANES), BF16) for c in groups]
    scratch += [vmem((2, count[c], chunk[c], LANES), F32) for c in groups]
    scratch += [vmem((SLOTS, plan.length[c][2] - 1, count[c], 8, LANES), BF16) for c in groups]
    scratch += [vmem((SLOTS, count[c], piece[c], LANES), BF16) for c in groups]
    scratch += [vmem((SLOTS, count[c], piece[c], LANES), F32) for c in groups]
    scratch += [vmem((4, 8, 8, LANES), F32)]
    scratch += [dma((len(plan.keys), SLOTS)), dma((len(plan.keys), SLOTS)), dma((4,)), dma((4,))]
    state, turned = vmem((tokens, width), BF16), vmem((width, tokens), BF16)
    scratch += [state, state, state, state, turned, turned, vmem((tokens, width), F32)]
    scratch += [vmem((tokens, hidden), BF16), vmem((tokens, W), BF16), vmem((tokens, W), BF16), vmem((hidden, width), BF16)]
    scratch += [vmem((4, width, W), BF16), vmem((4, width, W), BF16), vmem((4, W, width), BF16), dma((3 + tokens // min(256, tokens),)), dma((4, 3))]
    flops = 34 * tokens * width * hidden
    return pl.pallas_call(
        functools.partial(train_kernel, plan),
        name="gradients",
        out_shape=(pltpu.VMEM((tiles, 3, 2 * half, LANES), BF16), jax.ShapeDtypeStruct((8, LANES), F32)),
        in_specs=[pl.BlockSpec(memory_space=pl.ANY)] * 5,
        out_specs=(pl.BlockSpec(memory_space=pltpu.VMEM), pl.BlockSpec(memory_space=pltpu.VMEM)),
        scratch_shapes=scratch,
        cost_estimate=pl.CostEstimate(flops=flops, bytes_accessed=12 * width * hidden * 2, transcendentals=0),
        compiler_params=pltpu.CompilerParams(collective_id=0, has_side_effects=True, vmem_limit_bytes=48_000_000),
    )(x, dy, *weights)


def adamw_kernel(count, squares_ref, g_ref, *refs):
    ws, ms, vs, new_ws, new_ms, new_vs = (refs[i : i + 3] for i in range(0, 18, 3))
    factor = jnp.minimum(1.0, 0.5 * lax.rsqrt(jnp.sum(squares_ref[...]) / count + 1e-30))
    step = pl.program_id(0)
    per, half, lines = g_ref.shape[0] // 2, g_ref.shape[2] // 2, ms[0].shape[1]
    first, at = div(step, per) * per, rem(step, per)

    def update(color, g, rows, columns):
        g = g.astype(F32) * factor
        m = 0.9 * ms[color][0, rows, columns] + 0.1 * g
        v = 0.95 * vs[color][0, rows, columns] + 0.05 * g * g
        w = ws[color][0, rows, columns].astype(F32)
        new_ws[color][0, rows, columns] = (w - 0.02 * (m * lax.rsqrt(v + 1e-8) + 0.1 * w)).astype(BF16)
        new_ms[color][0, rows, columns] = m
        new_vs[color][0, rows, columns] = v

    for color in range(2):
        for t in range(per):
            for block in range(2):
                g = g_ref[first + t, color, pl.ds(pl.multiple_of(block * half + at * lines, 8), lines), :]
                update(color, g, slice(None), pl.ds((2 * t + block) * LANES, LANES))
    for block in range(2):
        update(2, g_ref[step, 2, pl.ds(block * half, half), :].astype(F32).T, pl.ds(block * LANES, LANES), slice(None))


def adamw(g, squares, weights, m, v):
    tiles, half = g.shape[0], g.shape[2] // 2
    per = tiles // 2
    up = pl.BlockSpec((1, half // per, W * per), lambda i: (1 - i // per, i % per, 0))
    down = pl.BlockSpec((1, W, half), lambda i: (1 - i // per, i % per, 0))
    three = [up, up, down]
    out = [jax.ShapeDtypeStruct(a.shape, a.dtype) for a in (*weights, *m, *v)]
    return pl.pallas_call(
        functools.partial(adamw_kernel, float(sum(w.size for w in weights))),
        name="adamw",
        grid=(tiles,),
        out_shape=out,
        in_specs=[pl.BlockSpec(squares.shape, lambda i: (0, 0)), pl.BlockSpec(memory_space=pltpu.VMEM)] + three * 3,
        out_specs=three * 3,
        compiler_params=pltpu.CompilerParams(vmem_limit_bytes=48_000_000),
    )(squares, pltpu.with_memory_space_constraint(g, pltpu.VMEM), *weights, *m, *v)


def solution(mesh):
    plan = Plan((4, 4, 8), 16, 768)

    def step(x, dy, *arrays):
        weights, m, v = (arrays[i : i + 3] for i in (0, 3, 6))
        g, squares = gradients(plan, x, dy, weights)
        return tuple(adamw(g, squares, weights, m, v))

    return jax.shard_map(
        step,
        mesh=mesh,
        in_specs=(P(("rep", "dp"), None, None),) * 2 + (P(None, None, None),) * 9,
        out_specs=(P("rep", None, None),) * 9,
        check_vma=False,
    )
```
